32 devices in a mesh: attn: 4 (over y, x), expert: 8 (over z, core).
Axes of the slice: x: 2, y: 2, z: 4, core: 2. Of those that a mesh axis runs over, the one named last changes fastest.
Arguments:
- tokens: bfloat16 [1024, 2880], P(('attn', 'expert')), may hold values from -6 to 6
- expert_ids: int32 [1024, 4], P(('attn', 'expert')), may hold values from 0 to 7, all different within a row; in each aligned block of 32 rows (0 to 31, 32 to 63, ...) at most 32 rows name the same one
- gate_probs: float32 [1024, 4], P(('attn', 'expert')), may hold values from 0.05 to 0.6
- shed_blocks: int32 [8], replicated, may hold values from 0 to 4, as said below
- partner: int32 [8], replicated, may hold values from 0 to 7, as said below
- gate_weight: bfloat16 [8, 2880, 2880], P('expert', None, 'attn'), may hold values from -0.109375 to 0.109375
- up_weight: bfloat16 [8, 2880, 2880], P('expert', None, 'attn'), may hold values from -0.109375 to 0.109375
- down_weight: bfloat16 [8, 2880, 2880], P('expert', 'attn'), may hold values from -0.109375 to 0.109375
Outputs:
- moe_out: bfloat16 [1024, 2880], P(('attn', 'expert'))
The draws below stay inside these ranges and needn't reach their ends.
Inputs may be any that keep to these rules, and one draw needn't show every extreme that they name: `expert_ids`: in the rows of one device, no expert is named by more than 32 rows; the 4 experts of a token differ. `shed_blocks`: some expert has exactly 4. partner pairs the experts: partner[partner[e]] = e and partner[e] != e.
All inputs are finite; a program needn't handle non-finite values.
Results may differ from the reference program's by a relative error of at most 0.0081.
Values may be sent and summed in bfloat16 or wider, within the bound.
A program may use at most 128 MiB of HBM per device.

```python
import math
import jax
import jax.numpy as jnp
import numpy as np
from jax import lax

D = 2880
FF = 2880
TOP = 4
SHED_MOST = 4
TOK_DEV = 32
TOKENS = 1024
EXPERTS = 8
MOST = 32
N_ATTN = 4


def draw_shed_blocks(key, part):
    first = jax.random.fold_in(key, 11)
    second = jax.random.fold_in(key, 12)
    values = jax.random.randint(first, (EXPERTS,), 0, SHED_MOST + 1).astype(jnp.int32)
    chosen = jax.random.randint(second, (), 0, EXPERTS)
    return values.at[chosen].set(SHED_MOST).astype(jnp.int32)


def draw_partner(key, part):
    shuffled = jax.random.permutation(jax.random.fold_in(key, 21), EXPERTS).astype(jnp.int32)
    left_side = shuffled[0::2]
    right_side = shuffled[1::2]
    paired = jnp.zeros((EXPERTS,), jnp.int32).at[left_side].set(right_side).at[right_side].set(left_side)
    return paired.astype(jnp.int32)


def block_scale(stream_key, shape, pieces, least, high):
    factor_of, own = 1.0, jax.random.fold_in(stream_key, 6)
    for dim, shards_of in pieces:
        draws = jnp.exp(jax.random.uniform(jax.random.fold_in(own, dim), (shards_of,), jnp.float32, least / len(pieces), high / len(pieces)))
        factor_of = factor_of * jnp.repeat(draws, shape[dim] // shards_of).reshape([-1 if axis == dim else 1 for axis in range(len(shape))])
    return factor_of


def routed_block(key, own, number, rows, number_of, top, most, skew):
    ranking = jax.random.permutation(key, number_of)
    heavy_load, common = load_shares(number_of, rows * top, most, skew, True), load_shares(number_of, rows * top, most, skew, False)
    places = jnp.arange(number_of)

    def named(lengths, rotation):
        used = int((lengths > 0).sum())
        fixed = max(1, used // 4)
        shifted = fixed + (places - fixed + rotation * (used - fixed)) % max(1, number_of - fixed)
        return jnp.zeros((number_of,), jnp.int32).at[ranking[jnp.where(places < fixed, places, shifted)]].set(jnp.asarray(lengths, jnp.int32))

    lengths = jnp.where(number % 4 == 0, named(heavy_load, number // 4), named(common, number - number // 4 - 1))
    mixed = jax.random.permutation(jax.random.fold_in(own, 3), number_of)
    source_of, receiver = mixed[0:number_of // 2 * 2:2], mixed[1:number_of // 2 * 2:2]
    margin = jnp.minimum(lengths[source_of] - 1, most - lengths[receiver]) // 2
    margin = jnp.where((source_of == ranking[0]) | (receiver == ranking[0]) | (lengths[receiver] == 0), 0, jnp.maximum(margin, 0))
    shifted = jax.random.randint(jax.random.fold_in(own, 4), (number_of // 2,), 0, 1 << 20) % (margin + 1)
    lengths = lengths.at[source_of].add(-shifted).at[receiver].add(shifted)
    labels = jnp.searchsorted(jnp.cumsum(lengths), jnp.arange(rows * top), side="right").astype(jnp.int32)
    listing = labels.reshape(top, rows).T
    listing = listing[jax.random.permutation(jax.random.fold_in(own, 1), rows)]
    rotation = jax.random.randint(jax.random.fold_in(own, 2), (rows, 1), 0, top)
    return jnp.take_along_axis(listing, (jnp.arange(top)[None, :] + rotation) % top, axis=1)


def load_shares(amount, total, reach, slope, full):
    portions = [(1 << 20) // math.isqrt(standing ** slope) + 1 for standing in range(1, amount + 1)]
    largest = reach if full else min(reach, max(-(-total // amount), total * portions[0] // sum(portions)))
    least = 1 if total - largest >= amount - 1 else 0
    holding, spare = [largest] + [least] * (amount - 1), total - largest - least * (amount - 1)
    while spare > 0:
        free = [i for i in range(1, amount) if holding[i] < largest] or [i for i in range(1, amount) if holding[i] < reach]
        pool, remaining = sum([portions[i] for i in free]), spare
        for i in free:
            addition = min(reach - holding[i], max(1, remaining * portions[i] // pool), spare)
            holding[i] = holding[i] + addition
            spare = spare - addition
    return np.array(holding)


def gaussian(key, extent, scale, most, cuts=(), kind=jnp.bfloat16):
    drawn = jax.random.normal(key, extent, jnp.float32) * scale
    if len(cuts) > 0:
        drawn = block_scale(key, extent, cuts, -0.22, 0.18) * drawn
    return jnp.clip(drawn, min=-most, max=most).astype(kind)


def setup_inputs(seed: int = 0) -> dict:
    streams_of = jax.random.split(jax.random.key(seed), 9)
    tokens = gaussian(streams_of[0], (TOKENS, D), 1.0, 6.0, ((0, 32),))
    expert_ids_keys = jax.random.split(jax.random.fold_in(streams_of[1], 1), TOKENS // TOK_DEV)
    expert_ids_turns = jax.random.permutation(jax.random.fold_in(streams_of[1], 3), TOKENS // TOK_DEV)
    expert_ids = jax.vmap(lambda own, number: routed_block(jax.random.fold_in(streams_of[1], 2), own, number, TOK_DEV, EXPERTS, TOP, MOST, 2))(expert_ids_keys, expert_ids_turns).reshape((TOKENS, TOP))
    gate_probs = jnp.clip(jnp.exp(math.log(0.6) - 2.4849067 * jax.random.uniform(streams_of[2], (TOKENS, TOP), jnp.float32) ** block_scale(streams_of[2], (TOKENS, TOP), ((0, 32),), -0.2, 0.2)), 0.05, 0.6)
    shed_blocks = draw_shed_blocks(jax.random.fold_in(streams_of[8], 71), 0)
    partner = draw_partner(jax.random.fold_in(streams_of[8], 71), 0)
    gate_weight = gaussian(streams_of[5], (EXPERTS, D, FF), D ** -0.5, 0.109375, ((0, 8), (2, 4)))
    up_weight = gaussian(streams_of[6], (EXPERTS, D, FF), D ** -0.5, 0.109375, ((0, 8), (2, 4)))
    down_weight = gaussian(streams_of[7], (EXPERTS, FF, D), FF ** -0.5, 0.109375, ((0, 8), (1, 4)))
    return {"tokens": tokens, "expert_ids": expert_ids, "gate_probs": gate_probs, "shed_blocks": shed_blocks, "partner": partner, "gate_weight": gate_weight, "up_weight": up_weight, "down_weight": down_weight}


SWISH_SCALE = 1.702


def activate(rows, gate_w, up_w):
    gate_part = jnp.dot(rows, gate_w, preferred_element_type=jnp.float32)
    up_part = jnp.dot(rows, up_w, preferred_element_type=jnp.float32)
    return (gate_part * jax.nn.sigmoid(SWISH_SCALE * gate_part) * (up_part + 1.0)).astype(jnp.bfloat16)


def reference(tokens, expert_ids, gate_probs, shed_blocks, partner, gate_weight, up_weight, down_weight):
    capacity = TOK_DEV * TOP * N_ATTN
    block_size = capacity // 8
    flat_ids = expert_ids.reshape(-1).astype(jnp.int32)
    onehot = (flat_ids[:, None] == jnp.arange(EXPERTS, dtype=jnp.int32)[None, :]).astype(jnp.int32)
    global_rank = jnp.sum((jnp.cumsum(onehot, axis=0) - onehot) * onehot, axis=1).astype(jnp.int32)
    limit = (capacity - block_size * shed_blocks[partner]).astype(jnp.int32)
    own_limit = limit[flat_ids]
    own_partner = partner[flat_ids].astype(jnp.int32)
    native = global_rank < own_limit
    borrowed = jnp.logical_and(jnp.logical_not(native), global_rank < own_limit + block_size * shed_blocks[flat_ids])
    target = jnp.where(native, flat_ids, jnp.where(borrowed, own_partner, -1)).astype(jnp.int32)
    slot_index = jnp.where(native, global_rank, limit[own_partner] + global_rank - own_limit).astype(jnp.int32)
    usable = target >= 0
    flat_index = jnp.where(usable, target * capacity + slot_index, EXPERTS * capacity).astype(jnp.int32)
    token_rows = jnp.repeat(tokens, TOP, axis=0)
    slot_rows = jnp.zeros((EXPERTS * capacity, D), jnp.bfloat16).at[flat_index].set(token_rows, mode="drop")
    slot_rows = slot_rows.reshape(EXPERTS, capacity, D)
    slot_place = jnp.arange(capacity, dtype=jnp.int32)

    def expert_layer(operands):
        rows, gate_w, up_w, down_w, other, bound = operands
        hidden_own = activate(rows, gate_w, up_w)
        hidden_other = activate(rows, gate_weight[other], up_weight[other])
        out_own = jnp.dot(hidden_own, down_w, preferred_element_type=jnp.float32)
        out_other = jnp.dot(hidden_other, down_weight[other], preferred_element_type=jnp.float32)
        keep = (slot_place < bound)[:, None]
        return jnp.where(keep, out_own, out_other).astype(jnp.bfloat16)

    expert_out = lax.map(expert_layer, (slot_rows, gate_weight, up_weight, down_weight, partner.astype(jnp.int32), limit))
    picked = expert_out.reshape(EXPERTS * capacity, D)[jnp.minimum(flat_index, EXPERTS * capacity - 1)]
    weights = jnp.where(usable, gate_probs.reshape(-1), 0.0).astype(jnp.float32)
    mixed = picked.astype(jnp.float32) * weights[:, None]
    return mixed.reshape(TOKENS, TOP, D).sum(axis=1).astype(jnp.bfloat16)
```

```python
import jax
import jax.numpy as jnp
from jax import lax
from jax.experimental import pallas as pl
from jax.experimental.pallas import tpu as pltpu
from jax.sharding import PartitionSpec as P

SHED_MOST = 4


SWISH_SCALE = 1.702
LANES = 128
VMEM_BYTES = 60 * 2**20
MESH = pl.DeviceIdType.MESH

OWN_XA, OWN_XB, OWN_YA, OWN_YB, OWN_C, FWD_Y, FWD_X, PASS_X, PASS_Y, PASS_D = range(10)
SUM_C, HALF_X, HALF_Y, FULL_XA, FULL_XB, FULL_YA, FULL_YB, BACK_Z, OUT_Z = range(10, 19)
META_Z, META_A, META_C = range(19, 22)
KINDS = 22


def lookup(table, indices):
    places = jnp.arange(table.shape[0], dtype=jnp.int32)
    return jnp.sum(jnp.where(indices[:, None] == places[None, :], table[None, :], 0), axis=1)


def served_rows(shed_blocks, partner, capacity):
    me = lax.axis_index("expert").astype(jnp.int32)[None]
    other = lookup(partner, me)
    block_size = capacity // 8
    return capacity + block_size * (lookup(shed_blocks, me) - lookup(shed_blocks, other))


def activate(gate_part, up_part, weight):
    return (gate_part * jax.nn.sigmoid(SWISH_SCALE * gate_part) * (up_part + 1.0) * weight).astype(
        jnp.bfloat16
    )


def kernel(
    tokens,
    ids,
    probs,
    shed,
    partner,
    gate_hbm,
    up_hbm,
    down_hbm,
    out,
    x,
    meta,
    m,
    wcol,
    part,
    core_in,
    total,
    half_in,
    full_in,
    z_out,
    z_in,
    kept,
    gate,
    up,
    down,
    hidden,
    send_sem,
    recv_sem,
    load_sem,
):
    planes = x.shape[0]
    rows, width = tokens.shape
    half = rows // 2
    top = ids.shape[0]
    capacity = rows * top * x.shape[2]
    a = lax.axis_index("attn")
    e = lax.axis_index("expert")
    z, c = e // 2, e % 2
    middle = (z + z // 2) % 2

    def xor(value, bits):
        result = value
        for bit in (1, 2, 4, 8):
            if bits & bit:
                result = result + bit - 2 * bit * ((value // bit) % 2)
        return result

    xn, yn, dn = xor(a, 1), xor(a, 2), xor(a, 3)
    oc = 1 - c
    to_x, to_y, to_d, to_c = (xn, e), (yn, e), (dn, e), (a, z * 2 + oc)

    def plane(s):
        low = (z % 2 + s % 2) % 2
        high = (z // 2 + s // 2) % 2
        return high * 2 + low

    def copy(kind, s, src, dst, to):
        return pltpu.make_async_remote_copy(
            src_ref=src,
            dst_ref=dst,
            send_sem=send_sem.at[kind, s],
            recv_sem=recv_sem.at[kind, s],
            device_id=to,
            device_id_type=MESH,
        )

    def same(kind, s, ref, to):
        return copy(kind, s, ref, ref, to)

    lo, hi = pl.ds(0, half), pl.ds(half, half)

    def make(kind, s):
        p = plane(s)
        if kind == OWN_XA:
            return same(kind, s, x.at[p, c, a, lo], to_x)
        if kind == OWN_XB:
            return same(kind, s, x.at[p, c, a, hi], to_x)
        if kind == OWN_YA:
            return same(kind, s, x.at[p, c, a, hi], to_y)
        if kind == OWN_YB:
            return same(kind, s, x.at[p, c, a, lo], to_y)
        if kind == OWN_C:
            return same(kind, s, x.at[p, c, a], to_c)
        if kind == FWD_Y:
            return same(kind, s, x.at[p, c, xn, lo], to_y)
        if kind == FWD_X:
            return same(kind, s, x.at[p, c, yn, hi], to_x)
        if kind == PASS_X:
            return same(kind, s, x.at[p, c, xn], to_c)
        if kind == PASS_Y:
            return same(kind, s, x.at[p, c, yn], to_c)
        if kind == PASS_D:
            return same(kind, s, x.at[p, c, dn], to_c)
        if kind == SUM_C:
            return copy(kind, s, part.at[s, oc], core_in.at[s], to_c)
        if kind == HALF_X:
            return copy(kind, s, total.at[s, dn, lo], half_in.at[s, 0], to_x)
        if kind == HALF_Y:
            return copy(kind, s, total.at[s, dn, hi], half_in.at[s, 1], to_y)
        if kind == FULL_XA:
            return copy(kind, s, total.at[s, xn, lo], full_in.at[s, 0, lo], to_x)
        if kind == FULL_XB:
            return copy(kind, s, total.at[s, xn, hi], full_in.at[s, 0, hi], to_x)
        if kind == FULL_YA:
            return copy(kind, s, total.at[s, yn, hi], full_in.at[s, 1, hi], to_y)
        if kind == FULL_YB:
            return copy(kind, s, total.at[s, yn, lo], full_in.at[s, 1, lo], to_y)
        if kind == BACK_Z:
            return copy(kind, s, z_out.at[s], z_in.at[s], (a, p * 2 + c))
        if kind == META_Z:
            return copy(kind, s, meta, m.at[a, z, c], (a, p * 2 + c))
        if kind == META_A:
            to = (to_x, to_x, to_y, to_d)[s]
            return same(kind, s, m.at[a, :, c], to)
        if kind == META_C:
            return same(kind, s, m.at[:, :, c], to_c)

    def hop(block, target):
        p = plane(block)
        return same(OUT_Z, block ^ target, x.at[p, c, a], (a, plane(target) * 2 + c))

    def start(s, *kinds):
        for kind in kinds:
            make(kind, s).start()

    def arrived(s, *kinds):
        for kind in kinds:
            make(kind, s).wait_recv()

    def sent(s, *kinds):
        for kind in kinds:
            make(kind, s).wait_send()

    def widen(ref):
        return ref[...].astype(jnp.float32)

    def at_middle(run):
        pl.when(middle == 1)(run)

    barrier = pltpu.get_barrier_semaphore()
    peers = [to_x, to_y, to_d, to_c] + [(a, plane(s) * 2 + c) for s in range(1, planes)]
    for peer in peers:
        pl.semaphore_signal(barrier, inc=1, device_id=peer, device_id_type=MESH)

    own = pltpu.make_async_copy(tokens, x.at[z, c, a], load_sem.at[3])
    own_meta = pltpu.make_async_copy(meta, m.at[a, z, c], load_sem.at[4])
    loads = [
        pltpu.make_async_copy(gate_hbm.at[0], gate, load_sem.at[0]),
        pltpu.make_async_copy(up_hbm.at[0], up, load_sem.at[1]),
        pltpu.make_async_copy(down_hbm.at[0], down, load_sem.at[2]),
    ]
    own.start()
    meta[...] = jnp.full(meta.shape, -1.0, jnp.float32)
    meta[:top, :rows] = ids[...].astype(jnp.float32)
    meta[top:, :rows] = probs[...]
    for load in loads:
        load.start()
    own.wait()
    own_meta.start()
    own_meta.wait()
    pl.semaphore_wait(barrier, len(peers))

    def share_own(s):
        start(s, OWN_XA, OWN_YA, OWN_XB, OWN_YB, OWN_C)

    def forward(s):
        arrived(s, OWN_XA)
        start(s, FWD_Y)
        arrived(s, OWN_YA)
        start(s, FWD_X)

    def pass_near(s):
        arrived(s, OWN_XB)
        start(s, PASS_X)
        arrived(s, OWN_YB)
        start(s, PASS_Y)

    def pass_far(s):
        arrived(s, FWD_Y, FWD_X)
        start(s, PASS_D)

    def ready(s):
        arrived(s, OWN_C, PASS_X, PASS_Y, PASS_D)

    def take(s):
        hop(0, s).wait_recv()

    def out_1():
        take(1)

        @at_middle
        def _():
            hop(1, 3).start()

        share_own(1)

        @at_middle
        def _():
            take(3)
            hop(3, 1).start()

    def out_2():
        take(2)

        @at_middle
        def _():
            hop(2, 1).start()

        share_own(2)

    def out_3():
        @pl.when(middle == 0)
        def _():
            take(3)

        share_own(3)

    for s in range(1, planes):
        start(s, META_Z)
    hop(0, 1).start()

    @at_middle
    def _():
        hop(0, 3).start()

    share_own(0)
    for s in range(1, planes):
        arrived(s, META_Z)
    for s in range(1, 4):
        start(s, META_A)

    def row_weights():
        table = m[...].reshape(m.shape[0] * m.shape[1] * m.shape[2], 2 * top, LANES)
        blocks = table.shape[0]
        named = table[:, :top, :] == e.astype(jnp.float32)
        mask = jnp.sum(jnp.where(named, 1.0, 0.0), axis=1)
        prob = jnp.sum(jnp.where(named, table[:, top:, :], 0.0), axis=1)
        mask16 = mask.astype(jnp.bfloat16)
        i = lax.broadcasted_iota(jnp.int32, (LANES, LANES), 0)
        j = lax.broadcasted_iota(jnp.int32, (LANES, LANES), 1)
        before = jnp.where(i < j, 1.0, 0.0).astype(jnp.bfloat16)
        inside = jnp.dot(mask16, before, preferred_element_type=jnp.float32)
        i = lax.broadcasted_iota(jnp.int32, (blocks, blocks), 0)
        j = lax.broadcasted_iota(jnp.int32, (blocks, blocks), 1)
        earlier = jnp.where(j < i, 1.0, 0.0).astype(jnp.bfloat16)
        ahead = jnp.dot(earlier, mask16, preferred_element_type=jnp.float32)
        rank = inside + jnp.sum(ahead, axis=1, keepdims=True)
        bound = capacity + capacity // 8 * (shed[e] - shed[partner[e]])
        weight = jnp.where(rank < bound.astype(jnp.float32), prob, 0.0)
        i = lax.broadcasted_iota(jnp.int32, (rows, LANES), 0)
        j = lax.broadcasted_iota(jnp.int32, (rows, LANES), 1)
        for aa in range(m.shape[0]):
            for zz in range(m.shape[1]):
                for cc in range(2):
                    block = (aa * m.shape[1] + zz) * 2 + cc
                    spread = jnp.where(i == j, weight[block : block + 1, :], 0.0)
                    wcol[zz, cc, aa] = jnp.sum(spread, axis=1, keepdims=True)

    count = 2 * x.shape[2] * rows
    along = (((1,), (1,)), ((), ()))
    units = gate.shape[0]

    def hidden_piece(s, cols):
        p = plane(s)
        xs = x[p].reshape(count, width)
        gate_part = lax.dot_general(xs, gate[cols], along, preferred_element_type=jnp.float32)
        up_part = lax.dot_general(xs, up[cols], along, preferred_element_type=jnp.float32)
        hidden[:, cols] = activate(gate_part, up_part, wcol[p].reshape(count, 1))

    def share_piece(s, cols):
        share = jnp.dot(hidden[...], down[:, cols], preferred_element_type=jnp.float32)
        part[s, :, :, :, cols] = share.astype(jnp.bfloat16).reshape(
            2, x.shape[2], rows, cols.stop - cols.start
        )

    def chunks(size, step):
        return [slice(first, min(first + step, size)) for first in range(0, size, step)]

    def core_sum(s, block, part_rows):
        return widen(part.at[s, c, block, part_rows]) + widen(core_in.at[s, block, part_rows])

    whole = pl.ds(0, rows)

    def begin(s):
        arrived(s, SUM_C)
        total[s, dn] = core_sum(s, dn, whole).astype(jnp.bfloat16)
        start(s, HALF_X, HALF_Y)
        total[s, xn, lo] = core_sum(s, xn, lo).astype(jnp.bfloat16)
        start(s, FULL_XA)
        total[s, yn, hi] = core_sum(s, yn, hi).astype(jnp.bfloat16)
        start(s, FULL_YA)

    def merge(s):
        arrived(s, HALF_X)
        low = core_sum(s, yn, lo) + widen(half_in.at[s, 0])
        total[s, yn, lo] = low.astype(jnp.bfloat16)
        start(s, FULL_YB)
        arrived(s, HALF_Y)
        high = core_sum(s, xn, hi) + widen(half_in.at[s, 1])
        total[s, xn, hi] = high.astype(jnp.bfloat16)
        start(s, FULL_XB)

    def finish(s):
        value = core_sum(s, a, whole)
        arrived(s, FULL_XA, FULL_YA, FULL_XB, FULL_YB)
        value = value + widen(full_in.at[s, 0]) + widen(full_in.at[s, 1])
        if s == 0:
            return value
        z_out[s] = value.astype(jnp.bfloat16)
        start(s, BACK_Z)

    def get_meta():
        for s in range(1, 4):
            arrived(s, META_A)
        start(0, META_C)

    def get_weights():
        arrived(0, META_C)
        row_weights()
        for load in loads:
            load.wait()

    call = lambda run, s: lambda: run(s)
    before = [
        call(forward, 0), get_meta, out_1, call(pass_near, 0), call(pass_far, 0), get_weights,
        call(ready, 0),
    ]
    for run in before:
        run()
    hooks = {
        (0, 1): [call(forward, 1)],
        (0, 4): [out_2],
        (0, 5): [call(pass_near, 1)],
        (1, 0): [call(pass_far, 1), call(ready, 1)],
        (1, 1): [call(forward, 2)],
        (1, 3): [out_3],
        (1, 5): [call(pass_near, 2)],
        (2, 0): [call(pass_far, 2), call(ready, 2)],
        (2, 1): [call(forward, 3), call(begin, 1)],
        (2, 5): [call(pass_near, 3)],
        (3, 0): [call(pass_far, 3), call(begin, 2), call(ready, 3)],
        (3, 4): [call(merge, 2)],
    }

    def hook(t, place):
        for step in range(planes):
            runs = hooks.get((step, place), [])

            def run_all(runs=runs):
                for run in runs:
                    run()

            if runs:
                pl.when(t == step)(run_all)

    def body(t, carry):
        place = 0
        for cols in chunks(units, 2 * LANES):
            hook(t, place)
            hidden_piece(t, cols)
            place += 1
        for cols in chunks(width, 8 * LANES):
            hook(t, place)
            share_piece(t, cols)
            place += 1
        start(t, SUM_C)
        return carry

    lax.fori_loop(0, planes, body, 0)
    begin(3)
    merge(3)
    merge(1)
    begin(0)
    finish(2)
    finish(3)
    merge(0)
    finish(1)
    value = finish(0)
    for s in (2, 3, 1):
        arrived(s, BACK_Z)
        value = value + widen(z_in.at[s])
    out[...] = value.astype(out.dtype)

    def drain(s, carry):
        sent(s, *range(OWN_XA, BACK_Z))

        @pl.when(s > 0)
        def _():
            sent(s, BACK_Z, META_Z)

        return carry

    lax.fori_loop(0, planes, drain, 0)
    hop(0, 1).wait_send()

    @at_middle
    def _():
        hop(0, 3).wait_send()
        hop(1, 3).wait_send()
        hop(2, 1).wait_send()
        hop(3, 1).wait_send()

    for s in range(1, 4):
        sent(s, META_A)
    sent(0, META_C)


def fused_bytes(group_count, planes, rows, width, hidden):
    wide = -(-width // LANES) * LANES
    block = rows * wide * 2
    weights = 2 * width * (-(-hidden // LANES) * LANES) * 2 + hidden * wide * 2
    return weights + planes * group_count * block * (2 + 2 + 1 + 1 + 2) + 12 * 2**20


def fused(tokens, ids, probs, shed, partner, gate_weight, up_weight, down_weight, group_count, planes):
    rows, width = tokens.shape
    hidden = gate_weight.shape[1]
    count = 2 * group_count * rows
    table = (2 * ids.shape[0], LANES)
    bf16, f32 = jnp.bfloat16, jnp.float32
    vmem = pl.BlockSpec(memory_space=pltpu.VMEM)
    smem = pl.BlockSpec(memory_space=pltpu.SMEM)
    hbm = pl.BlockSpec(memory_space=pl.ANY)
    return pl.pallas_call(
        kernel,
        out_shape=jax.ShapeDtypeStruct((rows, width), bf16),
        in_specs=[vmem, vmem, vmem, smem, smem, hbm, hbm, hbm],
        out_specs=vmem,
        scratch_shapes=[
            pltpu.VMEM((planes, 2, group_count, rows, width), bf16),
            pltpu.VMEM(table, f32),
            pltpu.VMEM((group_count, planes, 2) + table, f32),
            pltpu.VMEM((planes, 2, group_count, rows, 1), f32),
            pltpu.VMEM((planes, 2, group_count, rows, width), bf16),
            pltpu.VMEM((planes, group_count, rows, width), bf16),
            pltpu.VMEM((planes, group_count, rows, width), bf16),
            pltpu.VMEM((planes, 2, rows // 2, width), bf16),
            pltpu.VMEM((planes, 2, rows, width), bf16),
            pltpu.VMEM((planes, rows, width), bf16),
            pltpu.VMEM((planes, rows, width), bf16),
            pltpu.VMEM((rows, width), f32),
            pltpu.VMEM((hidden, width), bf16),
            pltpu.VMEM((hidden, width), bf16),
            pltpu.VMEM((hidden, width), bf16),
            pltpu.VMEM((count, hidden), bf16),
            pltpu.SemaphoreType.DMA((KINDS, planes)),
            pltpu.SemaphoreType.DMA((KINDS, planes)),
            pltpu.SemaphoreType.DMA((5,)),
        ],
        compiler_params=pltpu.CompilerParams(
            collective_id=0, has_side_effects=True, vmem_limit_bytes=VMEM_BYTES
        ),
    )(tokens, ids, probs, shed, partner, gate_weight, up_weight, down_weight)


def gathered(tokens, expert_ids, gate_probs, bound, gate_weight, up_weight, down_weight):
    both = ("attn", "expert")
    all_ids = lax.all_gather(expert_ids, both, axis=0, tiled=True)
    all_probs = lax.all_gather(gate_probs, both, axis=0, tiled=True)
    rows = lax.all_gather(tokens, both, axis=0, tiled=True)
    named = all_ids == lax.axis_index("expert").astype(jnp.int32)
    mask = jnp.any(named, axis=1).astype(jnp.int32)
    rank = jnp.cumsum(mask) - mask
    weight = jnp.sum(jnp.where(named, all_probs, 0.0), axis=1)
    weight = jnp.where(rank < bound, weight, 0.0)
    gate_part = jnp.dot(rows, gate_weight[0], preferred_element_type=jnp.float32)
    up_part = jnp.dot(rows, up_weight[0], preferred_element_type=jnp.float32)
    hidden = activate(gate_part, up_part, weight[:, None])
    share = jnp.dot(hidden, down_weight[0], preferred_element_type=jnp.float32).astype(jnp.bfloat16)
    share = lax.psum_scatter(share, "attn", scatter_dimension=0, tiled=True)
    return lax.psum_scatter(share, "expert", scatter_dimension=0, tiled=True)


def on_device(
    tokens, expert_ids, gate_probs, shed_blocks, partner, gate_weight, up_weight, down_weight
):
    rows, width = tokens.shape
    group_count, expert_count = lax.axis_size("attn"), lax.axis_size("expert")
    top_count = expert_ids.shape[1]
    planes = expert_count // 2
    fits = fused_bytes(group_count, planes, rows, width, gate_weight.shape[2]) <= VMEM_BYTES
    if group_count != 4 or planes != 4 or rows % 32 or rows > LANES or not fits:
        bound = served_rows(shed_blocks, partner, rows * top_count * group_count)
        return gathered(
            tokens, expert_ids, gate_probs, bound, gate_weight, up_weight, down_weight
        )
    return fused(
        tokens,
        expert_ids.T,
        gate_probs.T,
        shed_blocks,
        partner,
        jnp.swapaxes(gate_weight, 1, 2),
        jnp.swapaxes(up_weight, 1, 2),
        down_weight,
        group_count,
        planes,
    )


def solution(mesh):
    in_specs = (
        P(("attn", "expert"), None),
        P(("attn", "expert"), None),
        P(("attn", "expert"), None),
        P(),
        P(),
        P("expert", None, "attn"),
        P("expert", None, "attn"),
        P("expert", "attn", None),
    )
    out_specs = P(("attn", "expert"), None)
    return jax.shard_map(
        on_device, mesh=mesh, in_specs=in_specs, out_specs=out_specs, check_vma=False
    )
```

```python
import jax
import jax.numpy as jnp
from jax import lax
from jax.experimental import pallas as pl
from jax.experimental.pallas import tpu as pltpu
from jax.sharding import PartitionSpec as P

SHED_MOST = 4


SWISH_SCALE = 1.702
LANES = 128
VMEM_BYTES = 60 * 2**20
MESH = pl.DeviceIdType.MESH

OWN_XA, OWN_XB, OWN_YA, OWN_YB, OWN_C, FWD_Y, FWD_X, PASS_X, PASS_Y, PASS_D = range(10)
SUM_A, SUM_B, SUM_C, HALF_X, HALF_Y, FULL_XA, FULL_XB, FULL_YA, FULL_YB = range(10, 19)
BACK_Z, OUT_Z, META_Z, META_A, META_C = range(19, 24)
SUMS = (SUM_A, SUM_B, SUM_C)
KINDS = 24


def lookup(table, indices):
    places = jnp.arange(table.shape[0], dtype=jnp.int32)
    return jnp.sum(jnp.where(indices[:, None] == places[None, :], table[None, :], 0), axis=1)


def served_rows(shed_blocks, partner, capacity):
    me = lax.axis_index("expert").astype(jnp.int32)[None]
    other = lookup(partner, me)
    block_size = capacity // 8
    return capacity + block_size * (lookup(shed_blocks, me) - lookup(shed_blocks, other))


def activate(gate_part, up_part, weight):
    return (gate_part * jax.nn.sigmoid(SWISH_SCALE * gate_part) * (up_part + 1.0) * weight).astype(
        jnp.bfloat16
    )


def kernel(
    tokens,
    ids_hbm,
    probs_hbm,
    shed_hbm,
    partner_hbm,
    gate_hbm,
    up_hbm,
    down_hbm,
    out,
    x,
    ids,
    probs,
    shed,
    partner,
    m,
    wcol,
    part,
    core_in,
    total,
    half_in,
    full_in,
    z_out,
    z_in,
    kept,
    gate,
    up,
    down,
    hidden,
    send_sem,
    recv_sem,
    load_sem,
):
    planes = x.shape[0]
    rows, width = tokens.shape
    half = rows // 2
    top = ids.shape[0]
    capacity = rows * top * x.shape[2]
    a = lax.axis_index("attn")
    e = lax.axis_index("expert")
    z, c = e // 2, e % 2
    middle = (z + z // 2) % 2

    def xor(value, bits):
        result = value
        for bit in (1, 2, 4, 8):
            if bits & bit:
                result = result + bit - 2 * bit * ((value // bit) % 2)
        return result

    xn, yn, dn = xor(a, 1), xor(a, 2), xor(a, 3)
    oc = 1 - c
    to_x, to_y, to_d, to_c = (xn, e), (yn, e), (dn, e), (a, z * 2 + oc)

    def beyond(s):
        low = (z % 2 + s % 2) % 2
        high = (z // 2 + s // 2) % 2
        return high * 2 + low

    def apart(k):
        return k + middle * (k % 2) * (4 - 2 * k)

    def plane(k):
        return beyond(apart(k))

    def copy(kind, s, src, dst, to):
        return pltpu.make_async_remote_copy(
            src_ref=src,
            dst_ref=dst,
            send_sem=send_sem.at[kind, s],
            recv_sem=recv_sem.at[kind, s],
            device_id=to,
            device_id_type=MESH,
        )

    def same(kind, s, ref, to):
        return copy(kind, s, ref, ref, to)

    lo, hi = pl.ds(0, half), pl.ds(half, half)

    def chunks(size, step):
        return [slice(first, min(first + step, size)) for first in range(0, size, step)]

    lanes = -(-width // LANES)
    wide = chunks(width, -(-lanes // len(SUMS)) * LANES)

    def make(kind, s):
        if kind in (BACK_Z, META_Z):
            away = (a, beyond(s) * 2 + c)
        else:
            p = plane(s)
        if kind == OWN_XA:
            return same(kind, s, x.at[p, c, a, lo], to_x)
        if kind == OWN_XB:
            return same(kind, s, x.at[p, c, a, hi], to_x)
        if kind == OWN_YA:
            return same(kind, s, x.at[p, c, a, hi], to_y)
        if kind == OWN_YB:
            return same(kind, s, x.at[p, c, a, lo], to_y)
        if kind == OWN_C:
            return same(kind, s, x.at[p, c, a], to_c)
        if kind == FWD_Y:
            return same(kind, s, x.at[p, c, xn, lo], to_y)
        if kind == FWD_X:
            return same(kind, s, x.at[p, c, yn, hi], to_x)
        if kind == PASS_X:
            return same(kind, s, x.at[p, c, xn], to_c)
        if kind == PASS_Y:
            return same(kind, s, x.at[p, c, yn], to_c)
        if kind == PASS_D:
            return same(kind, s, x.at[p, c, dn], to_c)
        if kind in SUMS:
            cols = wide[SUMS.index(kind)]
            cols = pl.ds(cols.start, cols.stop - cols.start)
            return copy(kind, s, part.at[s, oc, :, :, cols], core_in.at[s, :, :, cols], to_c)
        if kind == HALF_X:
            return copy(kind, s, total.at[s, dn, lo], half_in.at[s, 0], to_x)
        if kind == HALF_Y:
            return copy(kind, s, total.at[s, dn, hi], half_in.at[s, 1], to_y)
        if kind == FULL_XA:
            return copy(kind, s, total.at[s, xn, lo], full_in.at[s, 0, lo], to_x)
        if kind == FULL_XB:
            return copy(kind, s, total.at[s, xn, hi], full_in.at[s, 0, hi], to_x)
        if kind == FULL_YA:
            return copy(kind, s, total.at[s, yn, hi], full_in.at[s, 1, hi], to_y)
        if kind == FULL_YB:
            return copy(kind, s, total.at[s, yn, lo], full_in.at[s, 1, lo], to_y)
        if kind == BACK_Z:
            return copy(kind, s, z_out.at[s], z_in.at[s], away)
        if kind == META_Z:
            return same(kind, s, m.at[:, z, c], away)
        if kind == META_A:
            to = (to_x, to_x, to_y, to_d)[s]
            return same(kind, s, m.at[a, z, c], to)
        if kind == META_C:
            return same(kind, s, m.at[:, :, c], to_c)

    def hop(block, target):
        p = beyond(block)
        return same(OUT_Z, block ^ target, x.at[p, c, a], (a, beyond(target) * 2 + c))

    def start(s, *kinds):
        for kind in kinds:
            make(kind, s).start()

    def arrived(s, *kinds):
        for kind in kinds:
            make(kind, s).wait_recv()

    def sent(s, *kinds):
        for kind in kinds:
            make(kind, s).wait_send()

    def widen(ref):
        return ref[...].astype(jnp.float32)

    def at_middle(run):
        pl.when(middle == 1)(run)

    def at_end(run):
        pl.when(middle == 0)(run)

    barrier = pltpu.get_barrier_semaphore()
    peers = [to_x, to_y, to_d, to_c] + [(a, beyond(s) * 2 + c) for s in range(1, planes)]
    for peer in peers:
        pl.semaphore_signal(barrier, inc=1, device_id=peer, device_id_type=MESH)

    own = pltpu.make_async_copy(tokens, x.at[z, c, a], load_sem.at[3])
    small = [
        pltpu.make_async_copy(ids_hbm, ids, load_sem.at[4]),
        pltpu.make_async_copy(probs_hbm, probs, load_sem.at[5]),
        pltpu.make_async_copy(shed_hbm, shed, load_sem.at[6]),
        pltpu.make_async_copy(partner_hbm, partner, load_sem.at[7]),
    ]
    loads = [
        pltpu.make_async_copy(gate_hbm.at[0], gate, load_sem.at[0]),
        pltpu.make_async_copy(up_hbm.at[0], up, load_sem.at[1]),
        pltpu.make_async_copy(down_hbm.at[0], down, load_sem.at[2]),
    ]
    for load in [own] + small + loads:
        load.start()
    for load in small:
        load.wait()
    m[a, z, c] = jnp.full(m.shape[3:], -1.0, jnp.float32)
    m[a, z, c, :top, :rows] = ids[...].astype(jnp.float32)
    m[a, z, c, top:, :rows] = probs[...]
    own.wait()
    pl.semaphore_wait(barrier, len(peers))

    def share_own(s):
        start(s, OWN_XA, OWN_YA, OWN_XB, OWN_YB, OWN_C)

    def forward(s):
        arrived(s, OWN_XA)
        start(s, FWD_Y)
        arrived(s, OWN_YA)
        start(s, FWD_X)

    def pass_near(s):
        arrived(s, OWN_XB)
        start(s, PASS_X)
        arrived(s, OWN_YB)
        start(s, PASS_Y)

    def pass_far(s):
        arrived(s, FWD_Y, FWD_X)
        start(s, PASS_D)

    def ready(s):
        arrived(s, OWN_C, PASS_X, PASS_Y, PASS_D)

    def take(s):
        same(OUT_Z, s, x.at[beyond(s), c, a], to_c).wait_recv()

    def out_1():
        take(apart(1))

        @at_middle
        def _():
            hop(3, 1).start()

        share_own(1)

        @at_middle
        def _():
            take(1)
            hop(1, 3).start()

    def out_2():
        take(2)

        @at_middle
        def _():
            hop(2, 1).start()

        share_own(2)

    def out_3():
        @pl.when(middle == 0)
        def _():
            take(3)

        share_own(3)

    for s in range(1, 4):
        start(s, META_A)
    hop(0, 1).start()

    @at_middle
    def _():
        hop(0, 3).start()

    share_own(0)
    for s in range(1, 4):
        arrived(s, META_A)
    for s in range(1, planes):
        start(s, META_Z)

    def row_weights():
        table = m[...].reshape(m.shape[0] * m.shape[1] * m.shape[2], 2 * top, LANES)
        blocks = table.shape[0]
        named = table[:, :top, :] == e.astype(jnp.float32)
        mask = jnp.sum(jnp.where(named, 1.0, 0.0), axis=1)
        prob = jnp.sum(jnp.where(named, table[:, top:, :], 0.0), axis=1)
        mask16 = mask.astype(jnp.bfloat16)
        i = lax.broadcasted_iota(jnp.int32, (LANES, LANES), 0)
        j = lax.broadcasted_iota(jnp.int32, (LANES, LANES), 1)
        before = jnp.where(i < j, 1.0, 0.0).astype(jnp.bfloat16)
        inside = jnp.dot(mask16, before, preferred_element_type=jnp.float32)
        i = lax.broadcasted_iota(jnp.int32, (blocks, blocks), 0)
        j = lax.broadcasted_iota(jnp.int32, (blocks, blocks), 1)
        earlier = jnp.where(j < i, 1.0, 0.0).astype(jnp.bfloat16)
        ahead = jnp.dot(earlier, mask16, preferred_element_type=jnp.float32)
        rank = inside + jnp.sum(ahead, axis=1, keepdims=True)
        bound = capacity + capacity // 8 * (shed[e] - shed[partner[e]])
        weight = jnp.where(rank < bound.astype(jnp.float32), prob, 0.0)
        i = lax.broadcasted_iota(jnp.int32, (rows, LANES), 0)
        j = lax.broadcasted_iota(jnp.int32, (rows, LANES), 1)
        for aa in range(m.shape[0]):
            for zz in range(m.shape[1]):
                for cc in range(2):
                    block = (aa * m.shape[1] + zz) * 2 + cc
                    spread = jnp.where(i == j, weight[block : block + 1, :], 0.0)
                    wcol[zz, cc, aa] = jnp.sum(spread, axis=1, keepdims=True)

    count = 2 * x.shape[2] * rows
    along = (((1,), (1,)), ((), ()))
    units = gate.shape[0]

    def hidden_piece(s, cols):
        p = plane(s)
        xs = x[p].reshape(count, width)
        gate_part = lax.dot_general(xs, gate[cols], along, preferred_element_type=jnp.float32)
        up_part = lax.dot_general(xs, up[cols], along, preferred_element_type=jnp.float32)
        hidden[:, cols] = activate(gate_part, up_part, wcol[p].reshape(count, 1))

    def share_piece(s, cols):
        share = jnp.dot(hidden[...], down[:, cols], preferred_element_type=jnp.float32)
        part[s, :, :, :, cols] = share.astype(jnp.bfloat16).reshape(
            2, x.shape[2], rows, cols.stop - cols.start
        )

    def core_sum(s, block, part_rows):
        return widen(part.at[s, c, block, part_rows]) + widen(core_in.at[s, block, part_rows])

    whole = pl.ds(0, rows)

    def begin(s):
        arrived(s, *SUMS)
        total[s, dn] = core_sum(s, dn, whole).astype(jnp.bfloat16)
        start(s, HALF_X, HALF_Y)
        total[s, xn, lo] = core_sum(s, xn, lo).astype(jnp.bfloat16)
        start(s, FULL_XA)
        total[s, yn, hi] = core_sum(s, yn, hi).astype(jnp.bfloat16)
        start(s, FULL_YA)

    def merge(s):
        arrived(s, HALF_X)
        low = core_sum(s, yn, lo) + widen(half_in.at[s, 0])
        total[s, yn, lo] = low.astype(jnp.bfloat16)
        start(s, FULL_YB)
        arrived(s, HALF_Y)
        high = core_sum(s, xn, hi) + widen(half_in.at[s, 1])
        total[s, xn, hi] = high.astype(jnp.bfloat16)
        start(s, FULL_XB)

    def finish(s):
        value = core_sum(s, a, whole)
        arrived(s, FULL_XA, FULL_YA, FULL_XB, FULL_YB)
        value = value + widen(full_in.at[s, 0]) + widen(full_in.at[s, 1])
        if s == 0:
            return value
        away = apart(s)
        z_out[away] = value.astype(jnp.bfloat16)
        start(away, BACK_Z)

    def get_meta():
        for s in range(1, planes):
            arrived(s, META_Z)
        start(0, META_C)

    def get_weights():
        arrived(0, META_C)
        row_weights()
        for load in loads:
            load.wait()

    call = lambda run, s: lambda: run(s)
    middle_does = lambda *runs: lambda: at_middle(lambda: [run() for run in runs] and None)
    end_does = lambda *runs: lambda: at_end(lambda: [run() for run in runs] and None)
    before = [
        call(forward, 0), out_1, call(pass_near, 0), get_meta, call(pass_far, 0), get_weights,
        call(ready, 0),
    ]
    for run in before:
        run()
    hooks = {
        (0, 1): [call(forward, 1)],
        (0, 3): [out_2],
        (0, 4): [call(pass_near, 1)],
        (1, 0): [call(pass_far, 1), call(ready, 1)],
        (1, 1): [call(forward, 2)],
        (1, 3): [out_3],
        (1, 4): [call(pass_near, 2)],
        (2, 0): [call(pass_far, 2), call(ready, 2)],
        (2, 1): [call(forward, 3), call(begin, 1)],
        (2, 4): [call(pass_near, 3)],
        (3, 0): [call(pass_far, 3), call(ready, 3)],
        (3, 1): [end_does(call(begin, 2))],
        (3, 2): [middle_does(call(merge, 1), call(begin, 2))],
    }

    def hook(t, place):
        for step in range(planes):
            runs = hooks.get((step, place), [])

            def run_all(runs=runs):
                for run in runs:
                    run()

            if runs:
                pl.when(t == step)(run_all)

    def body(t, carry):
        place = 0
        for cols in chunks(units, 2 * LANES):
            hook(t, place)
            hidden_piece(t, cols)
            place += 1
        for kind, cols in zip(SUMS, wide):
            hook(t, place)
            share_piece(t, cols)
            start(t, kind)
            place += 1
        return carry

    lax.fori_loop(0, planes, body, 0)
    at_middle(lambda: finish(1))
    merge(2)
    begin(3)
    finish(2)
    merge(3)
    at_end(lambda: merge(1))
    begin(0)
    finish(3)
    at_end(lambda: finish(1))
    merge(0)
    value = finish(0)
    for s in (2, 3, 1):
        arrived(s, BACK_Z)
        value = value + widen(z_in.at[s])
    out[...] = value.astype(out.dtype)

    def drain(s, carry):
        sent(s, *range(OWN_XA, BACK_Z))

        @pl.when(s > 0)
        def _():
            sent(s, BACK_Z, META_Z)

        return carry

    lax.fori_loop(0, planes, drain, 0)
    hop(0, 1).wait_send()

    @at_middle
    def _():
        hop(0, 3).wait_send()
        hop(1, 3).wait_send()
        hop(2, 1).wait_send()
        hop(3, 1).wait_send()

    for s in range(1, 4):
        sent(s, META_A)
    sent(0, META_C)


def fused_bytes(group_count, planes, rows, width, hidden):
    wide = -(-width // LANES) * LANES
    block = rows * wide * 2
    weights = 2 * width * (-(-hidden // LANES) * LANES) * 2 + hidden * wide * 2
    return weights + planes * group_count * block * (2 + 2 + 1 + 1 + 2) + 12 * 2**20


def fused(tokens, ids, probs, shed, partner, gate_weight, up_weight, down_weight, group_count, planes):
    rows, width = tokens.shape
    hidden = gate_weight.shape[1]
    count = 2 * group_count * rows
    table = (2 * ids.shape[0], LANES)
    bf16, f32 = jnp.bfloat16, jnp.float32
    vmem = pl.BlockSpec(memory_space=pltpu.VMEM)
    hbm = pl.BlockSpec(memory_space=pl.ANY)
    return pl.pallas_call(
        kernel,
        out_shape=pltpu.VMEM((rows, width), bf16),
        in_specs=[hbm] * 8,
        out_specs=vmem,
        scratch_shapes=[
            pltpu.VMEM((planes, 2, group_count, rows, width), bf16),
            pltpu.VMEM(ids.shape, ids.dtype),
            pltpu.VMEM(probs.shape, probs.dtype),
            pltpu.SMEM(shed.shape, shed.dtype),
            pltpu.SMEM(partner.shape, partner.dtype),
            pltpu.VMEM((group_count, planes, 2) + table, f32),
            pltpu.VMEM((planes, 2, group_count, rows, 1), f32),
            pltpu.VMEM((planes, 2, group_count, rows, width), bf16),
            pltpu.VMEM((planes, group_count, rows, width), bf16),
            pltpu.VMEM((planes, group_count, rows, width), bf16),
            pltpu.VMEM((planes, 2, rows // 2, width), bf16),
            pltpu.VMEM((planes, 2, rows, width), bf16),
            pltpu.VMEM((planes, rows, width), bf16),
            pltpu.VMEM((planes, rows, width), bf16),
            pltpu.VMEM((rows, width), f32),
            pltpu.VMEM((hidden, width), bf16),
            pltpu.VMEM((hidden, width), bf16),
            pltpu.VMEM((hidden, width), bf16),
            pltpu.VMEM((count, hidden), bf16),
            pltpu.SemaphoreType.DMA((KINDS, planes)),
            pltpu.SemaphoreType.DMA((KINDS, planes)),
            pltpu.SemaphoreType.DMA((8,)),
        ],
        compiler_params=pltpu.CompilerParams(
            collective_id=0, has_side_effects=True, vmem_limit_bytes=VMEM_BYTES
        ),
    )(tokens, ids, probs, shed, partner, gate_weight, up_weight, down_weight)


def gathered(tokens, expert_ids, gate_probs, bound, gate_weight, up_weight, down_weight):
    both = ("attn", "expert")
    all_ids = lax.all_gather(expert_ids, both, axis=0, tiled=True)
    all_probs = lax.all_gather(gate_probs, both, axis=0, tiled=True)
    rows = lax.all_gather(tokens, both, axis=0, tiled=True)
    named = all_ids == lax.axis_index("expert").astype(jnp.int32)
    mask = jnp.any(named, axis=1).astype(jnp.int32)
    rank = jnp.cumsum(mask) - mask
    weight = jnp.sum(jnp.where(named, all_probs, 0.0), axis=1)
    weight = jnp.where(rank < bound, weight, 0.0)
    gate_part = jnp.dot(rows, gate_weight[0], preferred_element_type=jnp.float32)
    up_part = jnp.dot(rows, up_weight[0], preferred_element_type=jnp.float32)
    hidden = activate(gate_part, up_part, weight[:, None])
    share = jnp.dot(hidden, down_weight[0], preferred_element_type=jnp.float32).astype(jnp.bfloat16)
    share = lax.psum_scatter(share, "attn", scatter_dimension=0, tiled=True)
    return lax.psum_scatter(share, "expert", scatter_dimension=0, tiled=True)


def on_device(
    tokens, expert_ids, gate_probs, shed_blocks, partner, gate_weight, up_weight, down_weight
):
    rows, width = tokens.shape
    group_count, expert_count = lax.axis_size("attn"), lax.axis_size("expert")
    top_count = expert_ids.shape[1]
    planes = expert_count // 2
    fits = fused_bytes(group_count, planes, rows, width, gate_weight.shape[2]) <= VMEM_BYTES
    if group_count != 4 or planes != 4 or rows % 32 or rows > LANES or not fits:
        bound = served_rows(shed_blocks, partner, rows * top_count * group_count)
        return gathered(
            tokens, expert_ids, gate_probs, bound, gate_weight, up_weight, down_weight
        )
    return fused(
        tokens,
        expert_ids.T,
        gate_probs.T,
        shed_blocks,
        partner,
        jnp.swapaxes(gate_weight, 1, 2),
        jnp.swapaxes(up_weight, 1, 2),
        down_weight,
        group_count,
        planes,
    )


def solution(mesh):
    in_specs = (
        P(("attn", "expert"), None),
        P(("attn", "expert"), None),
        P(("attn", "expert"), None),
        P(),
        P(),
        P("expert", None, "attn"),
        P("expert", None, "attn"),
        P("expert", "attn", None),
    )
    out_specs = P(("attn", "expert"), None)
    return jax.shard_map(
        on_device, mesh=mesh, in_specs=in_specs, out_specs=out_specs, check_vma=False
    )
```

```python
import jax
import jax.numpy as jnp
from jax import lax
from jax.experimental import pallas as pl
from jax.experimental.pallas import tpu as pltpu
from jax.sharding import PartitionSpec as P

SHED_MOST = 4


SWISH_SCALE = 1.702
LANES = 128
VMEM_BYTES = 60 * 2**20
MESH = pl.DeviceIdType.MESH

OWN_XA, OWN_XB, OWN_YA, OWN_YB, OWN_C, FWD_Y, FWD_X, PASS_X, PASS_Y, PASS_D = range(10)
SUM_A, SUM_B, SUM_C, OUT_Z, BACK_Z, META_Z, META_A = range(10, 17)
HALF_X, HALF_Y, FULL_XA, FULL_XB, FULL_YA, FULL_YB, META_C = range(17, 24)
SUMS = (SUM_A, SUM_B, SUM_C)
ROWS = 17
ROW = {
    HALF_X: OWN_XA, HALF_Y: OWN_YA, FULL_XA: OWN_XB, FULL_YA: OWN_YB, FULL_XB: FWD_X,
    FULL_YB: FWD_Y, META_C: META_A,
}


def lookup(table, indices):
    places = jnp.arange(table.shape[0], dtype=jnp.int32)
    return jnp.sum(jnp.where(indices[:, None] == places[None, :], table[None, :], 0), axis=1)


def served_rows(shed_blocks, partner, capacity):
    me = lax.axis_index("expert").astype(jnp.int32)[None]
    other = lookup(partner, me)
    block_size = capacity // 8
    return capacity + block_size * (lookup(shed_blocks, me) - lookup(shed_blocks, other))


def activate(gate_part, up_part, weight):
    return (gate_part * jax.nn.sigmoid(SWISH_SCALE * gate_part) * (up_part + 1.0) * weight).astype(
        jnp.bfloat16
    )


def kernel(
    tokens,
    ids_hbm,
    probs_hbm,
    shed_hbm,
    partner_hbm,
    gate_hbm,
    up_hbm,
    down_hbm,
    out,
    x,
    ids,
    probs,
    shed,
    partner,
    m,
    wcol,
    part,
    core_in,
    total,
    half_in,
    full_in,
    z_out,
    z_in,
    kept,
    gate,
    up,
    down,
    hidden,
    send_sem,
    recv_sem,
    load_sem,
):
    planes = x.shape[0]
    rows, width = tokens.shape
    half = rows // 2
    top = ids.shape[0]
    capacity = rows * top * x.shape[2]
    a = lax.axis_index("attn")
    e = lax.axis_index("expert")
    z, c = e // 2, e % 2
    middle = (z + z // 2) % 2

    def xor(value, bits):
        result = value
        for bit in (1, 2, 4, 8):
            if bits & bit:
                result = result + bit - 2 * bit * ((value // bit) % 2)
        return result

    xn, yn, dn = xor(a, 1), xor(a, 2), xor(a, 3)
    oc = 1 - c
    to_x, to_y, to_d, to_c = (xn, e), (yn, e), (dn, e), (a, z * 2 + oc)

    def beyond(s):
        low = (z % 2 + s % 2) % 2
        high = (z // 2 + s // 2) % 2
        return high * 2 + low

    def apart(k):
        return k + middle * ((k + 1) % 3 + 1 - k) * ((k + 3) // 4)

    def plane(k):
        return beyond(apart(k))

    def copy(kind, s, src, dst, to):
        return pltpu.make_async_remote_copy(
            src_ref=src,
            dst_ref=dst,
            send_sem=send_sem.at[0],
            recv_sem=recv_sem.at[ROW.get(kind, kind), s],
            device_id=to,
            device_id_type=MESH,
        )

    def same(kind, s, ref, to):
        return copy(kind, s, ref, ref, to)

    lo, hi = pl.ds(0, half), pl.ds(half, half)

    def chunks(size, step):
        return [slice(first, min(first + step, size)) for first in range(0, size, step)]

    lanes = -(-width // LANES)
    wide = chunks(width, -(-lanes // len(SUMS)) * LANES)

    def make(kind, s):
        if kind in (BACK_Z, META_Z):
            away = (a, beyond(s) * 2 + c)
        else:
            p = plane(s)
        if kind == OWN_XA:
            return same(kind, s, x.at[p, c, a, lo], to_x)
        if kind == OWN_XB:
            return same(kind, s, x.at[p, c, a, hi], to_x)
        if kind == OWN_YA:
            return same(kind, s, x.at[p, c, a, hi], to_y)
        if kind == OWN_YB:
            return same(kind, s, x.at[p, c, a, lo], to_y)
        if kind == OWN_C:
            return same(kind, s, x.at[p, c, a], to_c)
        if kind == FWD_Y:
            return same(kind, s, x.at[p, c, xn, lo], to_y)
        if kind == FWD_X:
            return same(kind, s, x.at[p, c, yn, hi], to_x)
        if kind == PASS_X:
            return same(kind, s, x.at[p, c, xn], to_c)
        if kind == PASS_Y:
            return same(kind, s, x.at[p, c, yn], to_c)
        if kind == PASS_D:
            return same(kind, s, x.at[p, c, dn], to_c)
        if kind in SUMS:
            cols = wide[SUMS.index(kind)]
            cols = pl.ds(cols.start, cols.stop - cols.start)
            return copy(kind, s, part.at[s, oc, :, :, cols], core_in.at[s, :, :, cols], to_c)
        if kind == HALF_X:
            return copy(kind, s, total.at[s, dn, lo], half_in.at[s, 0], to_x)
        if kind == HALF_Y:
            return copy(kind, s, total.at[s, dn, hi], half_in.at[s, 1], to_y)
        if kind == FULL_XA:
            return copy(kind, s, total.at[s, xn, lo], full_in.at[s, 0, lo], to_x)
        if kind == FULL_XB:
            return copy(kind, s, total.at[s, xn, hi], full_in.at[s, 0, hi], to_x)
        if kind == FULL_YA:
            return copy(kind, s, total.at[s, yn, hi], full_in.at[s, 1, hi], to_y)
        if kind == FULL_YB:
            return copy(kind, s, total.at[s, yn, lo], full_in.at[s, 1, lo], to_y)
        if kind == BACK_Z:
            return copy(kind, s, z_out.at[s], z_in.at[s], away)
        if kind == META_Z:
            return same(kind, s, m.at[:, z, c], away)
        if kind == META_A:
            to = (to_x, to_x, to_y, to_d)[s]
            return same(kind, s, m.at[a, z, c], to)
        if kind == META_C:
            return same(kind, s, m.at[:, :, c], to_c)

    def hop(block, target):
        p = beyond(block)
        return same(OUT_Z, block ^ target, x.at[p, c, a], (a, beyond(target) * 2 + c))

    def start(s, *kinds):
        for kind in kinds:
            make(kind, s).start()

    def arrived(s, *kinds):
        for kind in kinds:
            make(kind, s).wait_recv()

    def sent(s, *kinds):
        for kind in kinds:
            make(kind, s).wait_send()

    def widen(ref):
        return ref[...].astype(jnp.float32)

    def at_middle(run):
        pl.when(middle == 1)(run)

    def at_end(run):
        pl.when(middle == 0)(run)

    barrier = pltpu.get_barrier_semaphore()
    peers = [to_x, to_y, to_d, to_c] + [(a, beyond(s) * 2 + c) for s in range(1, planes)]
    for peer in peers:
        pl.semaphore_signal(barrier, inc=1, device_id=peer, device_id_type=MESH)

    own = pltpu.make_async_copy(tokens, x.at[z, c, a], load_sem.at[3])
    small = [
        pltpu.make_async_copy(ids_hbm, ids, load_sem.at[4]),
        pltpu.make_async_copy(probs_hbm, probs, load_sem.at[5]),
        pltpu.make_async_copy(shed_hbm, shed, load_sem.at[6]),
        pltpu.make_async_copy(partner_hbm, partner, load_sem.at[7]),
    ]
    loads = [
        pltpu.make_async_copy(gate_hbm.at[0], gate, load_sem.at[0]),
        pltpu.make_async_copy(up_hbm.at[0], up, load_sem.at[1]),
        pltpu.make_async_copy(down_hbm.at[0], down, load_sem.at[2]),
    ]
    for load in [own] + small + loads:
        load.start()
    for load in small:
        load.wait()
    m[a, z, c] = jnp.full(m.shape[3:], -1.0, jnp.float32)
    m[a, z, c, :top, :rows] = ids[...].astype(jnp.float32)
    m[a, z, c, top:, :rows] = probs[...]
    own.wait()
    pl.semaphore_wait(barrier, len(peers))

    def share_own(s):
        start(s, OWN_XA, OWN_YA, OWN_XB, OWN_YB, OWN_C)

    def forward(s):
        arrived(s, OWN_XA)
        start(s, FWD_Y)
        arrived(s, OWN_YA)
        start(s, FWD_X)

    def pass_near(s):
        arrived(s, OWN_XB)
        start(s, PASS_X)
        arrived(s, OWN_YB)
        start(s, PASS_Y)

    def pass_far(s):
        arrived(s, FWD_Y, FWD_X)
        start(s, PASS_D)

    def ready(s):
        arrived(s, OWN_C, PASS_X, PASS_Y, PASS_D)

    def take(s):
        same(OUT_Z, s, x.at[beyond(s), c, a], to_c).wait_recv()

    def out_1():
        take(apart(1))

        @at_middle
        def _():
            hop(3, 1).start()

        share_own(1)

        @at_middle
        def _():
            take(1)
            hop(1, 3).start()

    def out_2():
        at_end(lambda: take(2))
        share_own(2)

    def relay_2():
        take(2)
        hop(2, 1).start()

    def out_3():
        @pl.when(middle == 0)
        def _():
            take(3)

        share_own(3)

    for s in range(1, 4):
        start(s, META_A)
    hop(0, 1).start()

    @at_middle
    def _():
        hop(0, 3).start()

    share_own(0)
    for s in range(1, 4):
        arrived(s, META_A)
    for s in range(1, planes):
        start(s, META_Z)

    def row_weights():
        table = m[...].reshape(m.shape[0] * m.shape[1] * m.shape[2], 2 * top, LANES)
        blocks = table.shape[0]
        named = table[:, :top, :] == e.astype(jnp.float32)
        mask = jnp.sum(jnp.where(named, 1.0, 0.0), axis=1)
        prob = jnp.sum(jnp.where(named, table[:, top:, :], 0.0), axis=1)
        mask16 = mask.astype(jnp.bfloat16)
        i = lax.broadcasted_iota(jnp.int32, (LANES, LANES), 0)
        j = lax.broadcasted_iota(jnp.int32, (LANES, LANES), 1)
        before = jnp.where(i < j, 1.0, 0.0).astype(jnp.bfloat16)
        inside = jnp.dot(mask16, before, preferred_element_type=jnp.float32)
        i = lax.broadcasted_iota(jnp.int32, (blocks, blocks), 0)
        j = lax.broadcasted_iota(jnp.int32, (blocks, blocks), 1)
        earlier = jnp.where(j < i, 1.0, 0.0).astype(jnp.bfloat16)
        ahead = jnp.dot(earlier, mask16, preferred_element_type=jnp.float32)
        rank = inside + jnp.sum(ahead, axis=1, keepdims=True)
        bound = capacity + capacity // 8 * (shed[e] - shed[partner[e]])
        weight = jnp.where(rank < bound.astype(jnp.float32), prob, 0.0)
        i = lax.broadcasted_iota(jnp.int32, (rows, LANES), 0)
        j = lax.broadcasted_iota(jnp.int32, (rows, LANES), 1)
        for aa in range(m.shape[0]):
            for zz in range(m.shape[1]):
                for cc in range(2):
                    block = (aa * m.shape[1] + zz) * 2 + cc
                    spread = jnp.where(i == j, weight[block : block + 1, :], 0.0)
                    wcol[zz, cc, aa] = jnp.sum(spread, axis=1, keepdims=True)

    count = 2 * x.shape[2] * rows
    along = (((1,), (1,)), ((), ()))
    units = gate.shape[0]

    def hidden_piece(s, cols):
        p = plane(s)
        xs = x[p].reshape(count, width)
        gate_part = lax.dot_general(xs, gate[cols], along, preferred_element_type=jnp.float32)
        up_part = lax.dot_general(xs, up[cols], along, preferred_element_type=jnp.float32)
        hidden[:, cols] = activate(gate_part, up_part, wcol[p].reshape(count, 1))

    def share_piece(s, cols):
        share = jnp.dot(hidden[...], down[:, cols], preferred_element_type=jnp.float32)
        part[s, :, :, :, cols] = share.astype(jnp.bfloat16).reshape(
            2, x.shape[2], rows, cols.stop - cols.start
        )

    def core_sum(s, block, part_rows):
        return widen(part.at[s, c, block, part_rows]) + widen(core_in.at[s, block, part_rows])

    whole = pl.ds(0, rows)

    def begin_half(s):
        arrived(s, *SUMS)
        total[s, dn] = core_sum(s, dn, whole).astype(jnp.bfloat16)
        start(s, HALF_X, HALF_Y)

    def begin_full(s):
        total[s, xn, lo] = core_sum(s, xn, lo).astype(jnp.bfloat16)
        start(s, FULL_XA)
        total[s, yn, hi] = core_sum(s, yn, hi).astype(jnp.bfloat16)
        start(s, FULL_YA)

    def begin(s):
        begin_half(s)
        begin_full(s)

    def merge(s):
        arrived(s, HALF_X)
        low = core_sum(s, yn, lo) + widen(half_in.at[s, 0])
        total[s, yn, lo] = low.astype(jnp.bfloat16)
        start(s, FULL_YB)
        arrived(s, HALF_Y)
        high = core_sum(s, xn, hi) + widen(half_in.at[s, 1])
        total[s, xn, hi] = high.astype(jnp.bfloat16)
        start(s, FULL_XB)

    def finish(s):
        value = core_sum(s, a, whole)
        arrived(s, FULL_XA, FULL_YA, FULL_XB, FULL_YB)
        value = value + widen(full_in.at[s, 0]) + widen(full_in.at[s, 1])
        if s == 0:
            return value
        away = apart(s)
        z_out[away] = value.astype(jnp.bfloat16)
        start(away, BACK_Z)

    def get_meta():
        for s in range(1, planes):
            arrived(s, META_Z)
        start(0, META_C)

    def get_weights():
        arrived(0, META_C)
        row_weights()
        for load in loads:
            load.wait()

    call = lambda run, s: lambda: run(s)
    middle_does = lambda *runs: lambda: at_middle(lambda: [run() for run in runs] and None)
    end_does = lambda *runs: lambda: at_end(lambda: [run() for run in runs] and None)
    before = [
        call(forward, 0), out_1, call(pass_near, 0), get_meta, call(pass_far, 0), get_weights,
        call(ready, 0),
    ]
    for run in before:
        run()
    hooks = {
        (0, 1): [call(forward, 1)],
        (0, 3): [out_2, middle_does(relay_2)],
        (0, 4): [call(pass_near, 1)],
        (1, 0): [call(pass_far, 1), call(ready, 1), call(forward, 2)],
        (1, 2): [out_3],
        (1, 3): [call(pass_near, 2)],
        (2, 0): [call(pass_far, 2), call(ready, 2), call(forward, 3)],
        (2, 1): [call(begin, 1)],
        (2, 3): [call(pass_near, 3)],
        (3, 0): [
            call(pass_far, 3), call(ready, 3), middle_does(call(merge, 1)), call(begin, 2),
        ],
        (3, 5): [end_does(call(merge, 2))],
    }

    def hook(t, place):
        for step in range(planes):
            runs = hooks.get((step, place), [])

            def run_all(runs=runs):
                for run in runs:
                    run()

            if runs:
                pl.when(t == step)(run_all)

    def body(t, carry):
        place = 0
        for cols in chunks(units, 2 * LANES):
            hook(t, place)
            hidden_piece(t, cols)
            place += 1
        for kind, cols in zip(SUMS, wide):
            hook(t, place)
            share_piece(t, cols)
            start(t, kind)
            place += 1
        return carry

    lax.fori_loop(0, planes, body, 0)
    at_middle(lambda: (finish(1), merge(2)) and None)
    begin(3)
    finish(2)
    merge(3)
    at_end(lambda: merge(1))
    begin(0)
    finish(3)
    at_end(lambda: finish(1))
    merge(0)
    value = finish(0)
    for s in (2, 3, 1):
        arrived(s, BACK_Z)
        value = value + widen(z_in.at[s])
    out[...] = value.astype(out.dtype)

    def drain(s, carry):
        sent(s, *range(OWN_XA, OUT_Z), *range(HALF_X, META_C))

        @pl.when(s > 0)
        def _():
            sent(s, BACK_Z, META_Z)

        return carry

    lax.fori_loop(0, planes, drain, 0)
    hop(0, 1).wait_send()

    @at_middle
    def _():
        hop(0, 3).wait_send()
        hop(1, 3).wait_send()
        hop(2, 1).wait_send()
        hop(3, 1).wait_send()

    for s in range(1, 4):
        sent(s, META_A)
    sent(0, META_C)


def fused_bytes(group_count, planes, rows, width, hidden):
    wide = -(-width // LANES) * LANES
    block = rows * wide * 2
    weights = 2 * width * (-(-hidden // LANES) * LANES) * 2 + hidden * wide * 2
    return weights + planes * group_count * block * (2 + 2 + 1 + 1 + 2) + 12 * 2**20


def fused(tokens, ids, probs, shed, partner, gate_weight, up_weight, down_weight, group_count, planes):
    rows, width = tokens.shape
    hidden = gate_weight.shape[1]
    count = 2 * group_count * rows
    table = (2 * ids.shape[0], LANES)
    bf16, f32 = jnp.bfloat16, jnp.float32
    vmem = pl.BlockSpec(memory_space=pltpu.VMEM)
    hbm = pl.BlockSpec(memory_space=pl.ANY)
    return pl.pallas_call(
        kernel,
        out_shape=pltpu.VMEM((rows, width), bf16),
        in_specs=[hbm] * 8,
        out_specs=vmem,
        scratch_shapes=[
            pltpu.VMEM((planes, 2, group_count, rows, width), bf16),
            pltpu.VMEM(ids.shape, ids.dtype),
            pltpu.VMEM(probs.shape, probs.dtype),
            pltpu.SMEM(shed.shape, shed.dtype),
            pltpu.SMEM(partner.shape, partner.dtype),
            pltpu.VMEM((group_count, planes, 2) + table, f32),
            pltpu.VMEM((planes, 2, group_count, rows, 1), f32),
            pltpu.VMEM((planes, 2, group_count, rows, width), bf16),
            pltpu.VMEM((planes, group_count, rows, width), bf16),
            pltpu.VMEM((planes, group_count, rows, width), bf16),
            pltpu.VMEM((planes, 2, rows // 2, width), bf16),
            pltpu.VMEM((planes, 2, rows, width), bf16),
            pltpu.VMEM((planes, rows, width), bf16),
            pltpu.VMEM((planes, rows, width), bf16),
            pltpu.VMEM((rows, width), f32),
            pltpu.VMEM((hidden, width), bf16),
            pltpu.VMEM((hidden, width), bf16),
            pltpu.VMEM((hidden, width), bf16),
            pltpu.VMEM((count, hidden), bf16),
            pltpu.SemaphoreType.DMA((1,)),
            pltpu.SemaphoreType.DMA((ROWS, planes)),
            pltpu.SemaphoreType.DMA((8,)),
        ],
        compiler_params=pltpu.CompilerParams(
            collective_id=0, has_side_effects=True, vmem_limit_bytes=VMEM_BYTES
        ),
    )(tokens, ids, probs, shed, partner, gate_weight, up_weight, down_weight)


def gathered(tokens, expert_ids, gate_probs, bound, gate_weight, up_weight, down_weight):
    both = ("attn", "expert")
    all_ids = lax.all_gather(expert_ids, both, axis=0, tiled=True)
    all_probs = lax.all_gather(gate_probs, both, axis=0, tiled=True)
    rows = lax.all_gather(tokens, both, axis=0, tiled=True)
    named = all_ids == lax.axis_index("expert").astype(jnp.int32)
    mask = jnp.any(named, axis=1).astype(jnp.int32)
    rank = jnp.cumsum(mask) - mask
    weight = jnp.sum(jnp.where(named, all_probs, 0.0), axis=1)
    weight = jnp.where(rank < bound, weight, 0.0)
    gate_part = jnp.dot(rows, gate_weight[0], preferred_element_type=jnp.float32)
    up_part = jnp.dot(rows, up_weight[0], preferred_element_type=jnp.float32)
    hidden = activate(gate_part, up_part, weight[:, None])
    share = jnp.dot(hidden, down_weight[0], preferred_element_type=jnp.float32).astype(jnp.bfloat16)
    share = lax.psum_scatter(share, "attn", scatter_dimension=0, tiled=True)
    return lax.psum_scatter(share, "expert", scatter_dimension=0, tiled=True)


def on_device(
    tokens, expert_ids, gate_probs, shed_blocks, partner, gate_weight, up_weight, down_weight
):
    rows, width = tokens.shape
    group_count, expert_count = lax.axis_size("attn"), lax.axis_size("expert")
    top_count = expert_ids.shape[1]
    planes = expert_count // 2
    fits = fused_bytes(group_count, planes, rows, width, gate_weight.shape[2]) <= VMEM_BYTES
    if group_count != 4 or planes != 4 or rows % 32 or rows > LANES or not fits:
        bound = served_rows(shed_blocks, partner, rows * top_count * group_count)
        return gathered(
            tokens, expert_ids, gate_probs, bound, gate_weight, up_weight, down_weight
        )
    return fused(
        tokens,
        expert_ids.T,
        gate_probs.T,
        shed_blocks,
        partner,
        jnp.swapaxes(gate_weight, 1, 2),
        jnp.swapaxes(up_weight, 1, 2),
        down_weight,
        group_count,
        planes,
    )


def solution(mesh):
    in_specs = (
        P(("attn", "expert"), None),
        P(("attn", "expert"), None),
        P(("attn", "expert"), None),
        P(),
        P(),
        P("expert", None, "attn"),
        P("expert", None, "attn"),
        P("expert", "attn", None),
    )
    out_specs = P(("attn", "expert"), None)
    return jax.shard_map(
        on_device, mesh=mesh, in_specs=in_specs, out_specs=out_specs, check_vma=False
    )
```

```python
import jax
import jax.numpy as jnp
from jax import lax
from jax.experimental import pallas as pl
from jax.experimental.pallas import tpu as pltpu
from jax.sharding import PartitionSpec as P

SHED_MOST = 4


SWISH_SCALE = 1.702
LANES = 128
VMEM_BYTES = 60 * 2**20
MESH = pl.DeviceIdType.MESH

OWN_XA, OWN_XB, OWN_YA, OWN_YB, OWN_C, FWD_Y, FWD_X, PASS_X, PASS_Y, PASS_D = range(10)
SUM_A, SUM_B, OUT_Z, BACK_Z, META_Z, META_A, LATE_X, LATE_Y, LATE_Z = range(10, 19)
ROWS = 19
HALF_X, HALF_Y, FULL_XA, FULL_XB, FULL_YA, FULL_YB, META_C, DIAG_Z = range(19, 27)
SUMS = (SUM_A, SUM_B)
ROW = {
    HALF_X: OWN_XA, HALF_Y: OWN_YA, FULL_XA: OWN_XB, FULL_YA: OWN_YB, FULL_XB: FWD_X,
    FULL_YB: FWD_Y, META_C: META_A, DIAG_Z: META_Z,
}
LATE_ROW = {
    HALF_X: PASS_X, HALF_Y: PASS_Y, FULL_XA: PASS_D, FULL_YA: OWN_C, FULL_XB: LATE_X,
    FULL_YB: LATE_Y, BACK_Z: LATE_Z, DIAG_Z: LATE_Z,
}


def lookup(table, indices):
    places = jnp.arange(table.shape[0], dtype=jnp.int32)
    return jnp.sum(jnp.where(indices[:, None] == places[None, :], table[None, :], 0), axis=1)


def served_rows(shed_blocks, partner, capacity):
    me = lax.axis_index("expert").astype(jnp.int32)[None]
    other = lookup(partner, me)
    block_size = capacity // 8
    return capacity + block_size * (lookup(shed_blocks, me) - lookup(shed_blocks, other))


def activate(gate_part, up_part, weight):
    return (gate_part * jax.nn.sigmoid(SWISH_SCALE * gate_part) * (up_part + 1.0) * weight).astype(
        jnp.bfloat16
    )


def kernel(
    tokens,
    ids_hbm,
    probs_hbm,
    shed_hbm,
    partner_hbm,
    gate_hbm,
    up_hbm,
    down_hbm,
    out,
    x,
    ids,
    probs,
    shed,
    partner,
    m,
    wcol,
    part,
    core_in,
    total,
    half_in,
    full_in,
    z_out,
    z_in,
    diag_in,
    gate,
    up,
    down,
    hidden,
    send_sem,
    recv_sem,
    load_sem,
):
    planes = x.shape[0]
    rows, width = tokens.shape
    half = rows // 2
    top = ids.shape[0]
    capacity = rows * top * x.shape[2]
    a = lax.axis_index("attn")
    e = lax.axis_index("expert")
    z, c = e // 2, e % 2
    middle = (z + z // 2) % 2

    def xor(value, bits):
        result = value
        for bit in (1, 2, 4, 8):
            if bits & bit:
                result = result + bit - 2 * bit * ((value // bit) % 2)
        return result

    xn, yn, dn = xor(a, 1), xor(a, 2), xor(a, 3)
    oc = 1 - c
    to_x, to_y, to_d, to_c = (xn, e), (yn, e), (dn, e), (a, z * 2 + oc)

    def beyond(s):
        low = (z % 2 + s % 2) % 2
        high = (z // 2 + s // 2) % 2
        return high * 2 + low

    def apart(k):
        inner = ((k + 1) % 3 + 1 - k) * ((k + 3) // 4)
        return k + middle * (inner + (z // 2) * (k // 2) * (5 - 2 * k))

    def plane(k):
        return beyond(apart(k))

    def copy(kind, s, src, dst, to, late=0):
        row = LATE_ROW[kind] if late else ROW.get(kind, kind)
        return pltpu.make_async_remote_copy(
            src_ref=src,
            dst_ref=dst,
            send_sem=send_sem.at[0],
            recv_sem=recv_sem.at[row, s],
            device_id=to,
            device_id_type=MESH,
        )

    def same(kind, s, ref, to):
        return copy(kind, s, ref, ref, to)

    lo, hi = pl.ds(0, half), pl.ds(half, half)

    def chunks(size, step):
        return [slice(first, min(first + step, size)) for first in range(0, size, step)]

    lanes = -(-width // LANES)
    wide = chunks(width, -(-lanes // len(SUMS)) * LANES)

    def make(kind, s, q=0):
        cols = pl.ds(wide[q].start, wide[q].stop - wide[q].start)
        if kind in (BACK_Z, META_Z):
            away = (a, beyond(s) * 2 + c)
        else:
            p = plane(s)
        if kind == OWN_XA:
            return same(kind, s, x.at[p, c, a, lo], to_x)
        if kind == OWN_XB:
            return same(kind, s, x.at[p, c, a, hi], to_x)
        if kind == OWN_YA:
            return same(kind, s, x.at[p, c, a, hi], to_y)
        if kind == OWN_YB:
            return same(kind, s, x.at[p, c, a, lo], to_y)
        if kind == OWN_C:
            return same(kind, s, x.at[p, c, a], to_c)
        if kind == FWD_Y:
            return same(kind, s, x.at[p, c, xn, lo], to_y)
        if kind == FWD_X:
            return same(kind, s, x.at[p, c, yn, hi], to_x)
        if kind == PASS_X:
            return same(kind, s, x.at[p, c, xn], to_c)
        if kind == PASS_Y:
            return same(kind, s, x.at[p, c, yn], to_c)
        if kind == PASS_D:
            return same(kind, s, x.at[p, c, dn], to_c)
        if kind in SUMS:
            cols = wide[SUMS.index(kind)]
            cols = pl.ds(cols.start, cols.stop - cols.start)
            return copy(kind, s, part.at[s, oc, :, :, cols], core_in.at[s, :, :, cols], to_c)
        if kind == DIAG_Z:
            to = (a, beyond(1) * 2 + c)
            return copy(kind, 0, total.at[s, dn, :, cols], diag_in.at[:, cols], to, q)
        if kind == HALF_X:
            return copy(kind, s, total.at[s, dn, lo, cols], half_in.at[s, 0, :, cols], to_x, q)
        if kind == HALF_Y:
            return copy(kind, s, total.at[s, dn, hi, cols], half_in.at[s, 1, :, cols], to_y, q)
        if kind == FULL_XA:
            return copy(kind, s, total.at[s, xn, lo, cols], full_in.at[s, 0, lo, cols], to_x, q)
        if kind == FULL_XB:
            return copy(kind, s, total.at[s, xn, hi, cols], full_in.at[s, 0, hi, cols], to_x, q)
        if kind == FULL_YA:
            return copy(kind, s, total.at[s, yn, hi, cols], full_in.at[s, 1, hi, cols], to_y, q)
        if kind == FULL_YB:
            return copy(kind, s, total.at[s, yn, lo, cols], full_in.at[s, 1, lo, cols], to_y, q)
        if kind == BACK_Z:
            return copy(kind, s, z_out.at[s, :, cols], z_in.at[s, :, cols], away, q)
        if kind == META_Z:
            return same(kind, s, m.at[:, z, c], away)
        if kind == META_A:
            to = (to_x, to_x, to_y, to_d)[s]
            return same(kind, s, m.at[a, z, c], to)
        if kind == META_C:
            return same(kind, s, m.at[:, :, c], to_c)

    def hop(block, target):
        p = beyond(block)
        return same(OUT_Z, block ^ target, x.at[p, c, a], (a, beyond(target) * 2 + c))

    def start(s, *kinds, q=0):
        for kind in kinds:
            make(kind, s, q).start()

    def arrived(s, *kinds, q=0):
        for kind in kinds:
            make(kind, s, q).wait_recv()

    def sent(s, *kinds, q=0):
        for kind in kinds:
            make(kind, s, q).wait_send()

    def widen(ref):
        return ref[...].astype(jnp.float32)

    def at_middle(run):
        pl.when(middle == 1)(run)

    def at_end(run):
        pl.when(middle == 0)(run)

    barrier = pltpu.get_barrier_semaphore()
    peers = [to_x, to_y, to_d, to_c] + [(a, beyond(s) * 2 + c) for s in range(1, planes)]
    for peer in peers:
        pl.semaphore_signal(barrier, inc=1, device_id=peer, device_id_type=MESH)

    own = pltpu.make_async_copy(tokens, x.at[z, c, a], load_sem.at[3])
    small = [
        pltpu.make_async_copy(ids_hbm, ids, load_sem.at[4]),
        pltpu.make_async_copy(probs_hbm, probs, load_sem.at[5]),
        pltpu.make_async_copy(shed_hbm, shed, load_sem.at[6]),
        pltpu.make_async_copy(partner_hbm, partner, load_sem.at[7]),
    ]
    loads = [
        pltpu.make_async_copy(gate_hbm.at[0], gate, load_sem.at[0]),
        pltpu.make_async_copy(up_hbm.at[0], up, load_sem.at[1]),
        pltpu.make_async_copy(down_hbm.at[0], down, load_sem.at[2]),
    ]
    for load in [own] + small + loads:
        load.start()
    for load in small:
        load.wait()
    m[a, z, c] = jnp.full(m.shape[3:], -1.0, jnp.float32)
    m[a, z, c, :top, :rows] = ids[...].astype(jnp.float32)
    m[a, z, c, top:, :rows] = probs[...]
    own.wait()
    pl.semaphore_wait(barrier, len(peers))

    def share_own(s):
        start(s, OWN_XA, OWN_YA, OWN_XB, OWN_YB, OWN_C)

    def forward(s):
        arrived(s, OWN_XA)
        start(s, FWD_Y)
        arrived(s, OWN_YA)
        start(s, FWD_X)

    def pass_near(s):
        arrived(s, OWN_XB)
        start(s, PASS_X)
        arrived(s, OWN_YB)
        start(s, PASS_Y)

    def pass_far(s):
        arrived(s, FWD_Y, FWD_X)
        start(s, PASS_D)

    def ready(s):
        arrived(s, OWN_C, PASS_X, PASS_Y, PASS_D)

    def take(s):
        same(OUT_Z, s, x.at[beyond(s), c, a], to_c).wait_recv()

    def out_1():
        take(apart(1))

        @at_middle
        def _():
            hop(3, 1).start()

        share_own(1)

        @at_middle
        def _():
            take(1)
            hop(1, 3).start()

    def out_2():
        def relay_2():
            take(2)
            hop(2, 1).start()

        at_end(lambda: take(2))
        pl.when(z == 2)(relay_2)
        share_own(2)
        pl.when(z == 1)(relay_2)

    def out_3():
        @pl.when(middle == 0)
        def _():
            take(3)

        share_own(3)

    for s in range(1, 4):
        start(s, META_A)
    hop(0, 1).start()

    @at_middle
    def _():
        hop(0, 3).start()

    share_own(0)
    for s in range(1, 4):
        arrived(s, META_A)
    for s in range(1, planes):
        start(s, META_Z)

    def row_weights():
        table = m[...].reshape(m.shape[0] * m.shape[1] * m.shape[2], 2 * top, LANES)
        blocks = table.shape[0]
        named = table[:, :top, :] == e.astype(jnp.float32)
        mask = jnp.sum(jnp.where(named, 1.0, 0.0), axis=1)
        prob = jnp.sum(jnp.where(named, table[:, top:, :], 0.0), axis=1)
        mask16 = mask.astype(jnp.bfloat16)
        i = lax.broadcasted_iota(jnp.int32, (LANES, LANES), 0)
        j = lax.broadcasted_iota(jnp.int32, (LANES, LANES), 1)
        before = jnp.where(i < j, 1.0, 0.0).astype(jnp.bfloat16)
        inside = jnp.dot(mask16, before, preferred_element_type=jnp.float32)
        i = lax.broadcasted_iota(jnp.int32, (blocks, blocks), 0)
        j = lax.broadcasted_iota(jnp.int32, (blocks, blocks), 1)
        earlier = jnp.where(j < i, 1.0, 0.0).astype(jnp.bfloat16)
        ahead = jnp.dot(earlier, mask16, preferred_element_type=jnp.float32)
        rank = inside + jnp.sum(ahead, axis=1, keepdims=True)
        bound = capacity + capacity // 8 * (shed[e] - shed[partner[e]])
        weight = jnp.where(rank < bound.astype(jnp.float32), prob, 0.0)
        i = lax.broadcasted_iota(jnp.int32, (rows, LANES), 0)
        j = lax.broadcasted_iota(jnp.int32, (rows, LANES), 1)
        for aa in range(m.shape[0]):
            for zz in range(m.shape[1]):
                for cc in range(2):
                    block = (aa * m.shape[1] + zz) * 2 + cc
                    spread = jnp.where(i == j, weight[block : block + 1, :], 0.0)
                    wcol[zz, cc, aa] = jnp.sum(spread, axis=1, keepdims=True)

    count = 2 * x.shape[2] * rows
    along = (((1,), (1,)), ((), ()))
    units = gate.shape[0]

    def hidden_piece(s, cols):
        p = plane(s)
        xs = x[p].reshape(count, width)
        gate_part = lax.dot_general(xs, gate[cols], along, preferred_element_type=jnp.float32)
        up_part = lax.dot_general(xs, up[cols], along, preferred_element_type=jnp.float32)
        hidden[:, cols] = activate(gate_part, up_part, wcol[p].reshape(count, 1))

    def share_piece(s, cols):
        share = jnp.dot(hidden[...], down[:, cols], preferred_element_type=jnp.float32)
        part[s, :, :, :, cols] = share.astype(jnp.bfloat16).reshape(
            2, x.shape[2], rows, cols.stop - cols.start
        )

    def core_sum(s, block, part_rows, q):
        cols = wide[q]
        return widen(part.at[s, c, block, part_rows, cols]) + widen(
            core_in.at[s, block, part_rows, cols]
        )

    whole = pl.ds(0, rows)

    def either(s, diagonal, plain):
        if s == 0:
            plain()
        elif s == 1:
            at_end(diagonal)
            at_middle(plain)
        else:
            pl.when(z == s - 1)(diagonal)
            pl.when(z != s - 1)(plain)

    def begin_half(s, q):
        cols = wide[q]
        arrived(s, SUMS[q])
        far = core_sum(s, dn, whole, q)
        if s == 0:
            arrived(0, DIAG_Z, q=q)
            far = far + widen(diag_in.at[:, cols])
        total[s, dn, :, cols] = far.astype(jnp.bfloat16)
        either(s, lambda: start(s, DIAG_Z, q=q), lambda: start(s, HALF_X, HALF_Y, q=q))

    def begin_full(s, q):
        cols = wide[q]
        total[s, xn, lo, cols] = core_sum(s, xn, lo, q).astype(jnp.bfloat16)
        start(s, FULL_XA, q=q)
        total[s, yn, hi, cols] = core_sum(s, yn, hi, q).astype(jnp.bfloat16)
        start(s, FULL_YA, q=q)

        def diagonal():
            total[s, yn, lo, cols] = core_sum(s, yn, lo, q).astype(jnp.bfloat16)
            start(s, FULL_YB, q=q)
            total[s, xn, hi, cols] = core_sum(s, xn, hi, q).astype(jnp.bfloat16)
            start(s, FULL_XB, q=q)

        either(s, diagonal, lambda: None)

    def begin(s):
        begin_half(s, 0)
        begin_full(s, 0)
        begin_half(s, 1)
        begin_full(s, 1)

    def merge(s, *pieces):
        def plain():
            for q in pieces or (0, 1):
                cols = wide[q]
                arrived(s, HALF_X, q=q)
                low = core_sum(s, yn, lo, q) + widen(half_in.at[s, 0, :, cols])
                total[s, yn, lo, cols] = low.astype(jnp.bfloat16)
                start(s, FULL_YB, q=q)
                arrived(s, HALF_Y, q=q)
                high = core_sum(s, xn, hi, q) + widen(half_in.at[s, 1, :, cols])
                total[s, xn, hi, cols] = high.astype(jnp.bfloat16)
                start(s, FULL_XB, q=q)

        either(s, lambda: None, plain)

    def finish(s, *pieces):
        for q in pieces or (0, 1):
            cols = wide[q]
            value = core_sum(s, a, whole, q)
            arrived(s, FULL_XA, FULL_YA, FULL_XB, FULL_YB, q=q)
            value = value + widen(full_in.at[s, 0, :, cols]) + widen(full_in.at[s, 1, :, cols])
            if s == 0:
                for far in (2, 3, 1):
                    arrived(far, BACK_Z, q=q)
                    value = value + widen(z_in.at[far, :, cols])
                out[:, cols] = value.astype(out.dtype)
            else:
                away = apart(s)
                z_out[away, :, cols] = value.astype(jnp.bfloat16)
                start(away, BACK_Z, q=q)

    def get_meta():
        for s in range(1, planes):
            arrived(s, META_Z)
        start(0, META_C)

    def get_weights():
        arrived(0, META_C)
        row_weights()
        for load in loads:
            load.wait()

    call = lambda run, s: lambda: run(s)
    middle_does = lambda *runs: lambda: at_middle(lambda: [run() for run in runs] and None)
    end_does = lambda *runs: lambda: at_end(lambda: [run() for run in runs] and None)
    before = [
        call(forward, 0), out_1, call(pass_near, 0), get_meta, call(pass_far, 0), get_weights,
        call(ready, 0),
    ]
    for run in before:
        run()
    hooks = {
        (0, 1): [call(forward, 1)],
        (0, 3): [out_2],
        (0, 4): [call(pass_near, 1)],
        (1, 0): [call(pass_far, 1), call(ready, 1), call(forward, 2)],
        (1, 2): [out_3],
        (1, 3): [call(pass_near, 2)],
        (2, 0): [call(pass_far, 2), call(ready, 2), call(forward, 3)],
        (2, 1): [call(begin, 1)],
        (2, 3): [call(pass_near, 3)],
        (3, 0): [
            call(pass_far, 3), call(ready, 3), middle_does(call(merge, 1)), call(begin, 2),
        ],
        (3, 4): [end_does(lambda: merge(2, 0))],
    }

    def hook(t, place):
        for step in range(planes):
            runs = hooks.get((step, place), [])

            def run_all(runs=runs):
                for run in runs:
                    run()

            if runs:
                pl.when(t == step)(run_all)

    def body(t, carry):
        place = 0
        for cols in chunks(units, 2 * LANES):
            hook(t, place)
            hidden_piece(t, cols)
            place += 1
        for kind, cols in zip(SUMS, wide):
            hook(t, place)
            share_piece(t, cols)
            start(t, kind)
            place += 1
        return carry

    lax.fori_loop(0, planes, body, 0)
    finish(1)
    at_end(lambda: merge(2, 1))
    pl.when(z == 2)(lambda: merge(2))
    begin_half(3, 0)
    begin_full(3, 0)
    begin_half(3, 1)
    finish(2)
    merge(3, 0)
    begin_full(3, 1)
    merge(3, 1)

    def finish_3():
        finish(3, 0)
        finish(3, 1)

    pl.when(z == planes - 1)(finish_3)
    begin(0)
    pl.when(z != planes - 1)(finish_3)
    merge(0)
    finish(0)

    def drain(s, carry):
        sent(s, *range(OWN_XA, OUT_Z))
        for q in range(len(SUMS)):
            sent(s, *range(HALF_X, META_C), q=q)

        @pl.when(s > 0)
        def _():
            sent(s, META_Z)
            for q in range(len(SUMS)):
                sent(s, BACK_Z, q=q)

        return carry

    lax.fori_loop(0, planes, drain, 0)
    hop(0, 1).wait_send()

    @at_middle
    def _():
        hop(0, 3).wait_send()
        hop(1, 3).wait_send()
        hop(2, 1).wait_send()
        hop(3, 1).wait_send()

    for s in range(1, 4):
        sent(s, META_A)
    sent(0, META_C)


def fused_bytes(group_count, planes, rows, width, hidden):
    wide = -(-width // LANES) * LANES
    block = rows * wide * 2
    weights = 2 * width * (-(-hidden // LANES) * LANES) * 2 + hidden * wide * 2
    return weights + planes * group_count * block * (2 + 2 + 1 + 1 + 2) + 12 * 2**20


def fused(tokens, ids, probs, shed, partner, gate_weight, up_weight, down_weight, group_count, planes):
    rows, width = tokens.shape
    hidden = gate_weight.shape[1]
    count = 2 * group_count * rows
    table = (2 * ids.shape[0], LANES)
    bf16, f32 = jnp.bfloat16, jnp.float32
    vmem = pl.BlockSpec(memory_space=pltpu.VMEM)
    hbm = pl.BlockSpec(memory_space=pl.ANY)
    return pl.pallas_call(
        kernel,
        out_shape=pltpu.VMEM((rows, width), bf16),
        in_specs=[hbm] * 8,
        out_specs=vmem,
        scratch_shapes=[
            pltpu.VMEM((planes, 2, group_count, rows, width), bf16),
            pltpu.VMEM(ids.shape, ids.dtype),
            pltpu.VMEM(probs.shape, probs.dtype),
            pltpu.SMEM(shed.shape, shed.dtype),
            pltpu.SMEM(partner.shape, partner.dtype),
            pltpu.VMEM((group_count, planes, 2) + table, f32),
            pltpu.VMEM((planes, 2, group_count, rows, 1), f32),
            pltpu.VMEM((planes, 2, group_count, rows, width), bf16),
            pltpu.VMEM((planes, group_count, rows, width), bf16),
            pltpu.VMEM((planes, group_count, rows, width), bf16),
            pltpu.VMEM((planes, 2, rows // 2, width), bf16),
            pltpu.VMEM((planes, 2, rows, width), bf16),
            pltpu.VMEM((planes, rows, width), bf16),
            pltpu.VMEM((planes, rows, width), bf16),
            pltpu.VMEM((rows, width), bf16),
            pltpu.VMEM((hidden, width), bf16),
            pltpu.VMEM((hidden, width), bf16),
            pltpu.VMEM((hidden, width), bf16),
            pltpu.VMEM((count, hidden), bf16),
            pltpu.SemaphoreType.DMA((1,)),
            pltpu.SemaphoreType.DMA((ROWS, planes)),
            pltpu.SemaphoreType.DMA((8,)),
        ],
        compiler_params=pltpu.CompilerParams(
            collective_id=0, has_side_effects=True, vmem_limit_bytes=VMEM_BYTES
        ),
    )(tokens, ids, probs, shed, partner, gate_weight, up_weight, down_weight)


def gathered(tokens, expert_ids, gate_probs, bound, gate_weight, up_weight, down_weight):
    both = ("attn", "expert")
    all_ids = lax.all_gather(expert_ids, both, axis=0, tiled=True)
    all_probs = lax.all_gather(gate_probs, both, axis=0, tiled=True)
    rows = lax.all_gather(tokens, both, axis=0, tiled=True)
    named = all_ids == lax.axis_index("expert").astype(jnp.int32)
    mask = jnp.any(named, axis=1).astype(jnp.int32)
    rank = jnp.cumsum(mask) - mask
    weight = jnp.sum(jnp.where(named, all_probs, 0.0), axis=1)
    weight = jnp.where(rank < bound, weight, 0.0)
    gate_part = jnp.dot(rows, gate_weight[0], preferred_element_type=jnp.float32)
    up_part = jnp.dot(rows, up_weight[0], preferred_element_type=jnp.float32)
    hidden = activate(gate_part, up_part, weight[:, None])
    share = jnp.dot(hidden, down_weight[0], preferred_element_type=jnp.float32).astype(jnp.bfloat16)
    share = lax.psum_scatter(share, "attn", scatter_dimension=0, tiled=True)
    return lax.psum_scatter(share, "expert", scatter_dimension=0, tiled=True)


def on_device(
    tokens, expert_ids, gate_probs, shed_blocks, partner, gate_weight, up_weight, down_weight
):
    rows, width = tokens.shape
    group_count, expert_count = lax.axis_size("attn"), lax.axis_size("expert")
    top_count = expert_ids.shape[1]
    planes = expert_count // 2
    fits = fused_bytes(group_count, planes, rows, width, gate_weight.shape[2]) <= VMEM_BYTES
    if group_count != 4 or planes != 4 or rows % 32 or rows > LANES or not fits:
        bound = served_rows(shed_blocks, partner, rows * top_count * group_count)
        return gathered(
            tokens, expert_ids, gate_probs, bound, gate_weight, up_weight, down_weight
        )
    return fused(
        tokens,
        expert_ids.T,
        gate_probs.T,
        shed_blocks,
        partner,
        jnp.swapaxes(gate_weight, 1, 2),
        jnp.swapaxes(up_weight, 1, 2),
        down_weight,
        group_count,
        planes,
    )


def solution(mesh):
    in_specs = (
        P(("attn", "expert"), None),
        P(("attn", "expert"), None),
        P(("attn", "expert"), None),
        P(),
        P(),
        P("expert", None, "attn"),
        P("expert", None, "attn"),
        P("expert", "attn", None),
    )
    out_specs = P(("attn", "expert"), None)
    return jax.shard_map(
        on_device, mesh=mesh, in_specs=in_specs, out_specs=out_specs, check_vma=False
    )
```

```python
import jax
import jax.numpy as jnp
from jax import lax
from jax.experimental import pallas as pl
from jax.experimental.pallas import tpu as pltpu
from jax.sharding import PartitionSpec as P

SHED_MOST = 4


SWISH_SCALE = 1.702
LANES = 128
VMEM_BYTES = 60 * 2**20
MESH = pl.DeviceIdType.MESH

OWN_XA, OWN_XB, OWN_YA, OWN_YB, OWN_C, FWD_Y, FWD_X, PASS_X, PASS_Y, PASS_D = range(10)
SUM_A, SUM_B, OUT_Z, BACK_Z, META_Z, META_A, LATE_X, LATE_Y, LATE_Z = range(10, 19)
ROWS = 19
HALF_X, HALF_Y, FULL_XA, FULL_XB, FULL_YA, FULL_YB, META_C, DIAG_Z, FEED_Z = range(19, 28)
SUMS = (SUM_A, SUM_B)
ROW = {
    HALF_X: OWN_XA, HALF_Y: OWN_YA, FULL_XA: OWN_XB, FULL_YA: OWN_YB, FULL_XB: FWD_X,
    FULL_YB: FWD_Y, META_C: META_A, DIAG_Z: META_Z, FEED_Z: OUT_Z,
}
LATE_ROW = {
    HALF_X: PASS_X, HALF_Y: PASS_Y, FULL_XA: PASS_D, FULL_YA: OWN_C, FULL_XB: LATE_X,
    FULL_YB: LATE_Y, BACK_Z: LATE_Z, DIAG_Z: LATE_Z,
}


def lookup(table, indices):
    places = jnp.arange(table.shape[0], dtype=jnp.int32)
    return jnp.sum(jnp.where(indices[:, None] == places[None, :], table[None, :], 0), axis=1)


def served_rows(shed_blocks, partner, capacity):
    me = lax.axis_index("expert").astype(jnp.int32)[None]
    other = lookup(partner, me)
    block_size = capacity // 8
    return capacity + block_size * (lookup(shed_blocks, me) - lookup(shed_blocks, other))


def activate(gate_part, up_part, weight):
    return (gate_part * jax.nn.sigmoid(SWISH_SCALE * gate_part) * (up_part + 1.0) * weight).astype(
        jnp.bfloat16
    )


def kernel(
    tokens,
    ids_hbm,
    probs_hbm,
    shed_hbm,
    partner_hbm,
    gate_hbm,
    up_hbm,
    down_hbm,
    out,
    x,
    ids,
    probs,
    shed,
    partner,
    m,
    wcol,
    part,
    core_in,
    total,
    half_in,
    full_in,
    z_out,
    z_in,
    diag_in,
    gate,
    up,
    down,
    hidden,
    send_sem,
    recv_sem,
    load_sem,
):
    planes = x.shape[0]
    rows, width = tokens.shape
    half = rows // 2
    top = ids.shape[0]
    capacity = rows * top * x.shape[2]
    a = lax.axis_index("attn")
    e = lax.axis_index("expert")
    z, c = e // 2, e % 2
    middle = (z + z // 2) % 2

    def xor(value, bits):
        result = value
        for bit in (1, 2, 4, 8):
            if bits & bit:
                result = result + bit - 2 * bit * ((value // bit) % 2)
        return result

    xn, yn, dn = xor(a, 1), xor(a, 2), xor(a, 3)
    oc = 1 - c
    to_x, to_y, to_d, to_c = (xn, e), (yn, e), (dn, e), (a, z * 2 + oc)

    def beyond(s):
        low = (z % 2 + s % 2) % 2
        high = (z // 2 + s // 2) % 2
        return high * 2 + low

    def apart(k):
        inner = ((k + 1) % 3 + 1 - k) * ((k + 3) // 4)
        return k + middle * (inner + (z // 2) * (k // 2) * (5 - 2 * k))

    def plane(k):
        return beyond(apart(k))

    def copy(kind, s, src, dst, to, late=0):
        row = LATE_ROW[kind] if late else ROW.get(kind, kind)
        return pltpu.make_async_remote_copy(
            src_ref=src,
            dst_ref=dst,
            send_sem=send_sem.at[0],
            recv_sem=recv_sem.at[row, s],
            device_id=to,
            device_id_type=MESH,
        )

    def same(kind, s, ref, to):
        return copy(kind, s, ref, ref, to)

    lo, hi = pl.ds(0, half), pl.ds(half, half)

    def chunks(size, step):
        return [slice(first, min(first + step, size)) for first in range(0, size, step)]

    lanes = -(-width // LANES)
    wide = chunks(width, -(-lanes // len(SUMS)) * LANES)

    def make(kind, s, q=0):
        cols = pl.ds(wide[q].start, wide[q].stop - wide[q].start)
        if kind in (BACK_Z, META_Z):
            away = (a, beyond(s) * 2 + c)
        else:
            p = plane(s)
        if kind == OWN_XA:
            return same(kind, s, x.at[p, c, a, lo], to_x)
        if kind == OWN_XB:
            return same(kind, s, x.at[p, c, a, hi], to_x)
        if kind == OWN_YA:
            return same(kind, s, x.at[p, c, a, hi], to_y)
        if kind == OWN_YB:
            return same(kind, s, x.at[p, c, a, lo], to_y)
        if kind == OWN_C:
            return same(kind, s, x.at[p, c, a], to_c)
        if kind == FWD_Y:
            return same(kind, s, x.at[p, c, xn, lo], to_y)
        if kind == FWD_X:
            return same(kind, s, x.at[p, c, yn, hi], to_x)
        if kind == PASS_X:
            return same(kind, s, x.at[p, c, xn], to_c)
        if kind == PASS_Y:
            return same(kind, s, x.at[p, c, yn], to_c)
        if kind == PASS_D:
            return same(kind, s, x.at[p, c, dn], to_c)
        if kind in SUMS:
            cols = wide[SUMS.index(kind)]
            cols = pl.ds(cols.start, cols.stop - cols.start)
            return copy(kind, s, part.at[s, oc, :, :, cols], core_in.at[s, :, :, cols], to_c)
        if kind == FEED_Z:
            return same(kind, 0, x.at[beyond(s), c, dn], (a, beyond(1) * 2 + c))
        if kind == DIAG_Z:
            to = (a, beyond(1) * 2 + c)
            return copy(kind, 0, total.at[s, dn, :, cols], diag_in.at[:, cols], to, q)
        if kind == HALF_X:
            return copy(kind, s, total.at[s, dn, lo, cols], half_in.at[s, 0, :, cols], to_x, q)
        if kind == HALF_Y:
            return copy(kind, s, total.at[s, dn, hi, cols], half_in.at[s, 1, :, cols], to_y, q)
        if kind == FULL_XA:
            return copy(kind, s, total.at[s, xn, lo, cols], full_in.at[s, 0, lo, cols], to_x, q)
        if kind == FULL_XB:
            return copy(kind, s, total.at[s, xn, hi, cols], full_in.at[s, 0, hi, cols], to_x, q)
        if kind == FULL_YA:
            return copy(kind, s, total.at[s, yn, hi, cols], full_in.at[s, 1, hi, cols], to_y, q)
        if kind == FULL_YB:
            return copy(kind, s, total.at[s, yn, lo, cols], full_in.at[s, 1, lo, cols], to_y, q)
        if kind == BACK_Z:
            return copy(kind, s, z_out.at[s, :, cols], z_in.at[s, :, cols], away, q)
        if kind == META_Z:
            return same(kind, s, m.at[:, z, c], away)
        if kind == META_A:
            to = (to_x, to_x, to_y, to_d)[s]
            return same(kind, s, m.at[a, z, c], to)
        if kind == META_C:
            return same(kind, s, m.at[:, :, c], to_c)

    def hop(block, target):
        p = beyond(block)
        return same(OUT_Z, block ^ target, x.at[p, c, a], (a, beyond(target) * 2 + c))

    def start(s, *kinds, q=0):
        for kind in kinds:
            make(kind, s, q).start()

    def arrived(s, *kinds, q=0):
        for kind in kinds:
            make(kind, s, q).wait_recv()

    def sent(s, *kinds, q=0):
        for kind in kinds:
            make(kind, s, q).wait_send()

    def widen(ref):
        return ref[...].astype(jnp.float32)

    def at_middle(run):
        pl.when(middle == 1)(run)

    def at_end(run):
        pl.when(middle == 0)(run)

    barrier = pltpu.get_barrier_semaphore()
    peers = [to_x, to_y, to_d, to_c] + [(a, beyond(s) * 2 + c) for s in range(1, planes)]
    for peer in peers:
        pl.semaphore_signal(barrier, inc=1, device_id=peer, device_id_type=MESH)

    own = pltpu.make_async_copy(tokens, x.at[z, c, a], load_sem.at[3])
    small = [
        pltpu.make_async_copy(ids_hbm, ids, load_sem.at[4]),
        pltpu.make_async_copy(probs_hbm, probs, load_sem.at[5]),
        pltpu.make_async_copy(shed_hbm, shed, load_sem.at[6]),
        pltpu.make_async_copy(partner_hbm, partner, load_sem.at[7]),
    ]
    loads = [
        pltpu.make_async_copy(gate_hbm.at[0], gate, load_sem.at[0]),
        pltpu.make_async_copy(up_hbm.at[0], up, load_sem.at[1]),
        pltpu.make_async_copy(down_hbm.at[0], down, load_sem.at[2]),
    ]
    for load in [own] + small + loads:
        load.start()
    for load in small:
        load.wait()
    m[a, z, c] = jnp.full(m.shape[3:], -1.0, jnp.float32)
    m[a, z, c, :top, :rows] = ids[...].astype(jnp.float32)
    m[a, z, c, top:, :rows] = probs[...]
    own.wait()
    pl.semaphore_wait(barrier, len(peers))

    def share_own(s):
        start(s, OWN_XA, OWN_YA, OWN_XB, OWN_YB, OWN_C)

    def unfed(s, run):
        if s < 2:
            run()
        else:
            pl.when(z != s - 1)(run)

    def fed(s, run):
        if s >= 2:
            pl.when(z == s - 1)(run)

    def forward(s):
        arrived(s, OWN_XA)
        unfed(s, lambda: start(s, FWD_Y))
        arrived(s, OWN_YA)
        unfed(s, lambda: start(s, FWD_X))

    def pass_near(s):
        arrived(s, OWN_XB)
        start(s, PASS_X)
        arrived(s, OWN_YB)
        start(s, PASS_Y)

    def pass_far(s):
        def plain():
            arrived(s, FWD_Y, FWD_X)
            start(s, PASS_D)

        unfed(s, plain)
        if s == 0:
            at_end(lambda: start(0, FEED_Z))

    def pass_fed(s):
        def near():
            arrived(1, FEED_Z)
            start(s, PASS_D)

        fed(s, near)

    def ready(s):
        arrived(s, OWN_C, PASS_X, PASS_Y, PASS_D)

    def take(s):
        same(OUT_Z, s, x.at[beyond(s), c, a], to_c).wait_recv()

    def out_1():
        take(apart(1))

        @at_middle
        def _():
            hop(3, 1).start()

        share_own(1)

        @at_middle
        def _():
            take(1)
            hop(1, 3).start()

    def out_2():
        def relay_2():
            take(2)
            hop(2, 1).start()

        at_end(lambda: take(2))
        pl.when(z == 2)(relay_2)
        share_own(2)
        pl.when(z == 1)(relay_2)

    def out_3():
        @pl.when(middle == 0)
        def _():
            take(3)

        share_own(3)

    for s in range(1, 4):
        start(s, META_A)
    hop(0, 1).start()

    @at_middle
    def _():
        hop(0, 3).start()

    share_own(0)
    for s in range(1, 4):
        arrived(s, META_A)
    for s in range(1, planes):
        start(s, META_Z)

    def row_weights():
        table = m[...].reshape(m.shape[0] * m.shape[1] * m.shape[2], 2 * top, LANES)
        blocks = table.shape[0]
        named = table[:, :top, :] == e.astype(jnp.float32)
        mask = jnp.sum(jnp.where(named, 1.0, 0.0), axis=1)
        prob = jnp.sum(jnp.where(named, table[:, top:, :], 0.0), axis=1)
        mask16 = mask.astype(jnp.bfloat16)
        i = lax.broadcasted_iota(jnp.int32, (LANES, LANES), 0)
        j = lax.broadcasted_iota(jnp.int32, (LANES, LANES), 1)
        before = jnp.where(i < j, 1.0, 0.0).astype(jnp.bfloat16)
        inside = jnp.dot(mask16, before, preferred_element_type=jnp.float32)
        i = lax.broadcasted_iota(jnp.int32, (blocks, blocks), 0)
        j = lax.broadcasted_iota(jnp.int32, (blocks, blocks), 1)
        earlier = jnp.where(j < i, 1.0, 0.0).astype(jnp.bfloat16)
        ahead = jnp.dot(earlier, mask16, preferred_element_type=jnp.float32)
        rank = inside + jnp.sum(ahead, axis=1, keepdims=True)
        bound = capacity + capacity // 8 * (shed[e] - shed[partner[e]])
        weight = jnp.where(rank < bound.astype(jnp.float32), prob, 0.0)
        i = lax.broadcasted_iota(jnp.int32, (rows, LANES), 0)
        j = lax.broadcasted_iota(jnp.int32, (rows, LANES), 1)
        for aa in range(m.shape[0]):
            for zz in range(m.shape[1]):
                for cc in range(2):
                    block = (aa * m.shape[1] + zz) * 2 + cc
                    spread = jnp.where(i == j, weight[block : block + 1, :], 0.0)
                    wcol[zz, cc, aa] = jnp.sum(spread, axis=1, keepdims=True)

    count = 2 * x.shape[2] * rows
    along = (((1,), (1,)), ((), ()))
    units = gate.shape[0]

    def hidden_piece(s, cols):
        p = plane(s)
        xs = x[p].reshape(count, width)
        gate_part = lax.dot_general(xs, gate[cols], along, preferred_element_type=jnp.float32)
        up_part = lax.dot_general(xs, up[cols], along, preferred_element_type=jnp.float32)
        hidden[:, cols] = activate(gate_part, up_part, wcol[p].reshape(count, 1))

    def share_piece(s, cols):
        share = jnp.dot(hidden[...], down[:, cols], preferred_element_type=jnp.float32)
        part[s, :, :, :, cols] = share.astype(jnp.bfloat16).reshape(
            2, x.shape[2], rows, cols.stop - cols.start
        )

    def core_sum(s, block, part_rows, q):
        cols = wide[q]
        return widen(part.at[s, c, block, part_rows, cols]) + widen(
            core_in.at[s, block, part_rows, cols]
        )

    whole = pl.ds(0, rows)

    def either(s, diagonal, plain):
        if s == 0:
            plain()
        elif s == 1:
            at_end(diagonal)
            at_middle(plain)
        else:
            pl.when(z == s - 1)(diagonal)
            pl.when(z != s - 1)(plain)

    def begin_half(s, q):
        cols = wide[q]
        arrived(s, SUMS[q])
        far = core_sum(s, dn, whole, q)
        if s == 0:
            arrived(0, DIAG_Z, q=q)
            far = far + widen(diag_in.at[:, cols])
        total[s, dn, :, cols] = far.astype(jnp.bfloat16)
        either(s, lambda: start(s, DIAG_Z, q=q), lambda: start(s, HALF_X, HALF_Y, q=q))

    def begin_full(s, q):
        cols = wide[q]
        total[s, xn, lo, cols] = core_sum(s, xn, lo, q).astype(jnp.bfloat16)
        start(s, FULL_XA, q=q)
        total[s, yn, hi, cols] = core_sum(s, yn, hi, q).astype(jnp.bfloat16)
        start(s, FULL_YA, q=q)

        def diagonal():
            total[s, yn, lo, cols] = core_sum(s, yn, lo, q).astype(jnp.bfloat16)
            start(s, FULL_YB, q=q)
            total[s, xn, hi, cols] = core_sum(s, xn, hi, q).astype(jnp.bfloat16)
            start(s, FULL_XB, q=q)

        either(s, diagonal, lambda: None)

    def begin(s):
        begin_half(s, 0)
        begin_half(s, 1)
        begin_full(s, 0)
        begin_full(s, 1)

    def merge(s, *pieces):
        def plain():
            for q in pieces or (0, 1):
                cols = wide[q]
                arrived(s, HALF_X, q=q)
                low = core_sum(s, yn, lo, q) + widen(half_in.at[s, 0, :, cols])
                total[s, yn, lo, cols] = low.astype(jnp.bfloat16)
                start(s, FULL_YB, q=q)
                arrived(s, HALF_Y, q=q)
                high = core_sum(s, xn, hi, q) + widen(half_in.at[s, 1, :, cols])
                total[s, xn, hi, cols] = high.astype(jnp.bfloat16)
                start(s, FULL_XB, q=q)

        either(s, lambda: None, plain)

    def finish(s, *pieces):
        for q in pieces or (0, 1):
            cols = wide[q]
            value = core_sum(s, a, whole, q)
            arrived(s, FULL_XA, FULL_YA, FULL_XB, FULL_YB, q=q)
            value = value + widen(full_in.at[s, 0, :, cols]) + widen(full_in.at[s, 1, :, cols])
            if s == 0:
                for far in (2, 3, 1):
                    arrived(far, BACK_Z, q=q)
                    value = value + widen(z_in.at[far, :, cols])
                out[:, cols] = value.astype(out.dtype)
            else:
                away = apart(s)
                z_out[away, :, cols] = value.astype(jnp.bfloat16)
                start(away, BACK_Z, q=q)

    def get_meta():
        for s in range(1, planes):
            arrived(s, META_Z)
        start(0, META_C)

    def get_weights():
        arrived(0, META_C)
        row_weights()
        for load in loads:
            load.wait()

    call = lambda run, s: lambda: run(s)
    middle_does = lambda *runs: lambda: at_middle(lambda: [run() for run in runs] and None)
    end_does = lambda *runs: lambda: at_end(lambda: [run() for run in runs] and None)
    before = [
        call(forward, 0), out_1, call(pass_near, 0), get_meta, call(pass_far, 0), get_weights,
        call(ready, 0),
    ]
    for run in before:
        run()
    hooks = {
        (0, 1): [call(forward, 1)],
        (0, 3): [out_2],
        (0, 4): [call(pass_near, 1)],
        (1, 0): [call(pass_far, 1), call(ready, 1), call(forward, 2)],
        (1, 2): [out_3],
        (1, 3): [call(pass_near, 2), call(pass_fed, 2)],
        (2, 0): [call(pass_far, 2), call(ready, 2), lambda: unfed(3, lambda: forward(3))],
        (2, 1): [call(begin, 1)],
        (2, 3): [lambda: fed(3, lambda: forward(3)), call(pass_near, 3), call(pass_fed, 3)],
        (3, 0): [
            middle_does(call(merge, 1)), call(pass_far, 3), call(ready, 3), call(begin, 2),
        ],
        (3, 2): [middle_does(call(finish, 1))],
        (3, 4): [end_does(lambda: merge(2, 0))],
    }

    def hook(t, place):
        for step in range(planes):
            runs = hooks.get((step, place), [])

            def run_all(runs=runs):
                for run in runs:
                    run()

            if runs:
                pl.when(t == step)(run_all)

    def body(t, carry):
        place = 0
        for cols in chunks(units, 2 * LANES):
            hook(t, place)
            hidden_piece(t, cols)
            place += 1
        for kind, cols in zip(SUMS, wide):
            hook(t, place)
            share_piece(t, cols)
            start(t, kind)
            place += 1
        return carry

    lax.fori_loop(0, planes, body, 0)
    at_end(lambda: finish(1))
    at_end(lambda: merge(2, 1))
    pl.when(z == 2)(lambda: merge(2))
    begin_half(3, 0)
    begin_full(3, 0)
    pl.when(z == 1)(lambda: finish(2))
    begin_half(3, 1)
    pl.when(z != 1)(lambda: finish(2))
    merge(3, 0)
    begin_full(3, 1)
    merge(3, 1)

    def finish_3():
        finish(3, 0)
        finish(3, 1)

    pl.when(z == planes - 1)(finish_3)
    begin(0)
    pl.when(z != planes - 1)(finish_3)
    merge(0)
    finish(0)

    def drain(s, carry):
        sent(s, *range(OWN_XA, FWD_Y), *range(PASS_X, OUT_Z))

        @pl.when(jnp.logical_or(middle == 0, apart(s) != 1))
        def _():
            sent(s, FWD_Y, FWD_X)

        for q in range(len(SUMS)):
            sent(s, *range(HALF_X, META_C), q=q)

        @pl.when(s > 0)
        def _():
            sent(s, META_Z)
            for q in range(len(SUMS)):
                sent(s, BACK_Z, q=q)

        return carry

    lax.fori_loop(0, planes, drain, 0)
    at_end(lambda: sent(0, FEED_Z))
    hop(0, 1).wait_send()

    @at_middle
    def _():
        hop(0, 3).wait_send()
        hop(1, 3).wait_send()
        hop(2, 1).wait_send()
        hop(3, 1).wait_send()

    for s in range(1, 4):
        sent(s, META_A)
    sent(0, META_C)


def fused_bytes(group_count, planes, rows, width, hidden):
    wide = -(-width // LANES) * LANES
    block = rows * wide * 2
    weights = 2 * width * (-(-hidden // LANES) * LANES) * 2 + hidden * wide * 2
    return weights + planes * group_count * block * (2 + 2 + 1 + 1 + 2) + 12 * 2**20


def fused(tokens, ids, probs, shed, partner, gate_weight, up_weight, down_weight, group_count, planes):
    rows, width = tokens.shape
    hidden = gate_weight.shape[1]
    count = 2 * group_count * rows
    table = (2 * ids.shape[0], LANES)
    bf16, f32 = jnp.bfloat16, jnp.float32
    vmem = pl.BlockSpec(memory_space=pltpu.VMEM)
    hbm = pl.BlockSpec(memory_space=pl.ANY)
    return pl.pallas_call(
        kernel,
        out_shape=pltpu.VMEM((rows, width), bf16),
        in_specs=[hbm] * 8,
        out_specs=vmem,
        scratch_shapes=[
            pltpu.VMEM((planes, 2, group_count, rows, width), bf16),
            pltpu.VMEM(ids.shape, ids.dtype),
            pltpu.VMEM(probs.shape, probs.dtype),
            pltpu.SMEM(shed.shape, shed.dtype),
            pltpu.SMEM(partner.shape, partner.dtype),
            pltpu.VMEM((group_count, planes, 2) + table, f32),
            pltpu.VMEM((planes, 2, group_count, rows, 1), f32),
            pltpu.VMEM((planes, 2, group_count, rows, width), bf16),
            pltpu.VMEM((planes, group_count, rows, width), bf16),
            pltpu.VMEM((planes, group_count, rows, width), bf16),
            pltpu.VMEM((planes, 2, rows // 2, width), bf16),
            pltpu.VMEM((planes, 2, rows, width), bf16),
            pltpu.VMEM((planes, rows, width), bf16),
            pltpu.VMEM((planes, rows, width), bf16),
            pltpu.VMEM((rows, width), bf16),
            pltpu.VMEM((hidden, width), bf16),
            pltpu.VMEM((hidden, width), bf16),
            pltpu.VMEM((hidden, width), bf16),
            pltpu.VMEM((count, hidden), bf16),
            pltpu.SemaphoreType.DMA((1,)),
            pltpu.SemaphoreType.DMA((ROWS, planes)),
            pltpu.SemaphoreType.DMA((8,)),
        ],
        compiler_params=pltpu.CompilerParams(
            collective_id=0, has_side_effects=True, vmem_limit_bytes=VMEM_BYTES
        ),
    )(tokens, ids, probs, shed, partner, gate_weight, up_weight, down_weight)


def gathered(tokens, expert_ids, gate_probs, bound, gate_weight, up_weight, down_weight):
    both = ("attn", "expert")
    all_ids = lax.all_gather(expert_ids, both, axis=0, tiled=True)
    all_probs = lax.all_gather(gate_probs, both, axis=0, tiled=True)
    rows = lax.all_gather(tokens, both, axis=0, tiled=True)
    named = all_ids == lax.axis_index("expert").astype(jnp.int32)
    mask = jnp.any(named, axis=1).astype(jnp.int32)
    rank = jnp.cumsum(mask) - mask
    weight = jnp.sum(jnp.where(named, all_probs, 0.0), axis=1)
    weight = jnp.where(rank < bound, weight, 0.0)
    gate_part = jnp.dot(rows, gate_weight[0], preferred_element_type=jnp.float32)
    up_part = jnp.dot(rows, up_weight[0], preferred_element_type=jnp.float32)
    hidden = activate(gate_part, up_part, weight[:, None])
    share = jnp.dot(hidden, down_weight[0], preferred_element_type=jnp.float32).astype(jnp.bfloat16)
    share = lax.psum_scatter(share, "attn", scatter_dimension=0, tiled=True)
    return lax.psum_scatter(share, "expert", scatter_dimension=0, tiled=True)


def on_device(
    tokens, expert_ids, gate_probs, shed_blocks, partner, gate_weight, up_weight, down_weight
):
    rows, width = tokens.shape
    group_count, expert_count = lax.axis_size("attn"), lax.axis_size("expert")
    top_count = expert_ids.shape[1]
    planes = expert_count // 2
    fits = fused_bytes(group_count, planes, rows, width, gate_weight.shape[2]) <= VMEM_BYTES
    if group_count != 4 or planes != 4 or rows % 32 or rows > LANES or not fits:
        bound = served_rows(shed_blocks, partner, rows * top_count * group_count)
        return gathered(
            tokens, expert_ids, gate_probs, bound, gate_weight, up_weight, down_weight
        )
    return fused(
        tokens,
        expert_ids.T,
        gate_probs.T,
        shed_blocks,
        partner,
        jnp.swapaxes(gate_weight, 1, 2),
        jnp.swapaxes(up_weight, 1, 2),
        down_weight,
        group_count,
        planes,
    )


def solution(mesh):
    in_specs = (
        P(("attn", "expert"), None),
        P(("attn", "expert"), None),
        P(("attn", "expert"), None),
        P(),
        P(),
        P("expert", None, "attn"),
        P("expert", None, "attn"),
        P("expert", "attn", None),
    )
    out_specs = P(("attn", "expert"), None)
    return jax.shard_map(
        on_device, mesh=mesh, in_specs=in_specs, out_specs=out_specs, check_vma=False
    )
```
